32 devices in a mesh: dp: 4 (over x, y), ep: 8 (over z, core).
Axes of the slice: x: 2, y: 2, z: 4, core: 2. Of those that a mesh axis runs over, the one named last changes fastest.
Arguments:
- x_a: bfloat16 [32768, 768], P(('dp', 'ep')), parts along dimension 0
- x_b: bfloat16 [32768, 768], P(('dp', 'ep')), parts along dimension 0
- dy_b: bfloat16 [32768, 768], P(('dp', 'ep')), parts along dimension 0
- w_q: bfloat16 [768, 768], replicated
- w_k: bfloat16 [768, 768], replicated
- w_v: bfloat16 [768, 768], replicated
- w_o: bfloat16 [768, 768], replicated
- gain_attn: float32 [768], replicated
- gain_moe: float32 [768], replicated
- w_gate: bfloat16 [8, 768, 3072], P('ep')
- w_up: bfloat16 [8, 768, 3072], P('ep')
- w_down: bfloat16 [8, 3072, 768], P('ep')
- expert_a: int32 [32768, 1], P(('dp', 'ep')), parts along dimension 0
- slot_a: int32 [32768, 1], P(('dp', 'ep')), parts along dimension 0
- gate_a: bfloat16 [32768, 1], P(('dp', 'ep')), parts along dimension 0
- expert_b: int32 [32768, 1], P(('dp', 'ep')), parts along dimension 0
- slot_b: int32 [32768, 1], P(('dp', 'ep')), parts along dimension 0
- gate_b: bfloat16 [32768, 1], P(('dp', 'ep')), parts along dimension 0
Outputs:
- output 1: bfloat16 [32768, 768], P(('dp', 'ep')), parts along dimension 0
- output 2: bfloat16 [32768, 768], P(('dp', 'ep')), parts along dimension 0
- output 3: float32 [3072, 768], P('dp'), parts along dimension 0
- output 4: float32 [3072, 768], P('dp'), parts along dimension 0
- output 5: float32 [3072, 768], P('dp'), parts along dimension 0
- output 6: float32 [3072, 768], P('dp'), parts along dimension 0
- output 7: float32 [32, 768, 3072], P(('dp', 'ep')), parts along dimension 0
- output 8: float32 [32, 768, 3072], P(('dp', 'ep')), parts along dimension 0
- output 9: float32 [32, 3072, 768], P(('dp', 'ep')), parts along dimension 0
There are 4 independent parts. The reference program is written for one: setup_inputs(seed, part) draws one part's arguments, and reference() takes and returns one part's arrays. A program takes and returns all parts, laid end to end along the dimension named above; an argument that names none is the same for every part.
All inputs are finite; a program needn't handle non-finite values.
Results may differ from the reference program's by a relative error of at most 0.0168784.
Values are sent between devices in bfloat16 or wider.
A program may use at most 1 GiB of HBM per device.

```python
import jax
import jax.numpy as jnp
from jax import lax

GROUP_SIZE = 8
TOKENS_DEV = 1024
MODEL_DIM = 768
EXPERTS = 8
FF_DIM = 3072
TOP_K = 1
HEAD_DIM = 128
NUM_HEADS = 6
SEQ_LEN = 256
CAPACITY = 384
RMS_EPS = 1e-6
ROWS_PART = GROUP_SIZE * TOKENS_DEV
NUM_SEQ = ROWS_PART // SEQ_LEN
SLOTS_EXPERT = GROUP_SIZE * CAPACITY


def draw_routing(key_route):
    key_noise, key_level, key_force = jax.random.split(key_route, 3)
    noise_int = jax.random.randint(key_noise, (GROUP_SIZE, TOKENS_DEV, EXPERTS), 0, 2 ** 16)
    levels = jax.random.randint(key_level, (EXPERTS,), 0, 3) * 2 ** 13
    forced = jax.random.randint(key_force, (GROUP_SIZE,), 0, EXPERTS)
    expert_iota = jnp.arange(EXPERTS)
    boosted = (jnp.arange(TOKENS_DEV)[None, :, None] < CAPACITY) & (expert_iota[None, None, :] == forced[:, None, None])
    scores = (noise_int + levels + jnp.where(boosted, 2 ** 18, 0)) * EXPERTS + expert_iota
    _, expert_ids = lax.top_k(scores, TOP_K)
    onehot = (expert_ids.reshape(GROUP_SIZE, TOKENS_DEV * TOP_K, 1) == expert_iota).astype(jnp.int32)
    slot_rank = jnp.sum((jnp.cumsum(onehot, axis=1) - 1) * onehot, axis=-1)
    slot_ids = jnp.where(slot_rank < CAPACITY, slot_rank, -1)
    return expert_ids.reshape(ROWS_PART, TOP_K).astype(jnp.int32), slot_ids.reshape(ROWS_PART, TOP_K).astype(jnp.int32)


def setup_inputs(seed: int = 0, part: int = 0) -> dict:
    root_key = jax.random.key(seed)
    key_shared, key_part = jax.random.split(root_key)
    shared = jax.random.split(key_shared, 9)
    local_keys = jax.random.split(jax.random.fold_in(key_part, part), 6)

    def normal(key_one, shape, scale):
        return (jax.random.normal(key_one, shape, jnp.float32) * scale).astype(jnp.bfloat16)

    attn_scale = MODEL_DIM ** -0.5
    expert_a, slot_a = draw_routing(local_keys[3])
    expert_b, slot_b = draw_routing(local_keys[4])
    gate_vals = jax.random.uniform(local_keys[5], (2, ROWS_PART, TOP_K), jnp.float32, 0.25, 1.0).astype(jnp.bfloat16)
    return {
        'x_a': normal(local_keys[0], (ROWS_PART, MODEL_DIM), 1.0),
        'x_b': normal(local_keys[1], (ROWS_PART, MODEL_DIM), 1.0),
        'dy_b': normal(local_keys[2], (ROWS_PART, MODEL_DIM), 1.0),
        'w_q': normal(shared[0], (MODEL_DIM, MODEL_DIM), attn_scale),
        'w_k': normal(shared[1], (MODEL_DIM, MODEL_DIM), attn_scale),
        'w_v': normal(shared[2], (MODEL_DIM, MODEL_DIM), attn_scale),
        'w_o': normal(shared[3], (MODEL_DIM, MODEL_DIM), attn_scale),
        'gain_attn': 1.0 + 0.3 * jax.random.normal(shared[4], (MODEL_DIM,), jnp.float32),
        'gain_moe': 1.0 + 0.3 * jax.random.normal(shared[5], (MODEL_DIM,), jnp.float32),
        'w_gate': normal(shared[6], (EXPERTS, MODEL_DIM, FF_DIM), attn_scale),
        'w_up': normal(shared[7], (EXPERTS, MODEL_DIM, FF_DIM), attn_scale),
        'w_down': normal(shared[8], (EXPERTS, FF_DIM, MODEL_DIM), FF_DIM ** -0.5),
        'expert_a': expert_a,
        'slot_a': slot_a,
        'gate_a': gate_vals[0],
        'expert_b': expert_b,
        'slot_b': slot_b,
        'gate_b': gate_vals[1],
    }


def rms_norm(row_block, gain_vec):
    rows_f = row_block.astype(jnp.float32)
    inv_rms = lax.rsqrt(jnp.mean(rows_f * rows_f, axis=-1, keepdims=True) + RMS_EPS)
    return (rows_f * inv_rms * gain_vec).astype(jnp.bfloat16)


def attention_block(x_rows, w_q, w_k, w_v, w_o, gain_attn):
    causal = jnp.arange(SEQ_LEN)[:, None] >= jnp.arange(SEQ_LEN)[None, :]

    def one_sequence(seq_rows):
        normed = rms_norm(seq_rows, gain_attn)

        def project(weight):
            return jnp.dot(normed, weight.astype(jnp.bfloat16), preferred_element_type=jnp.float32).astype(jnp.bfloat16).reshape(SEQ_LEN, NUM_HEADS, HEAD_DIM).astype(jnp.float32)

        scores = jnp.einsum('qhd,khd->hqk', project(w_q), project(w_k)) * HEAD_DIM ** -0.5
        attn_probs = jax.nn.softmax(jnp.where(causal, scores, -1e30), axis=-1).astype(jnp.bfloat16).astype(jnp.float32)
        mixed_rows = jnp.einsum('hqk,khd->qhd', attn_probs, project(w_v)).astype(jnp.bfloat16).reshape(SEQ_LEN, MODEL_DIM)
        return (seq_rows.astype(jnp.float32) + jnp.dot(mixed_rows, w_o.astype(jnp.bfloat16), preferred_element_type=jnp.float32)).astype(jnp.bfloat16)

    return lax.map(one_sequence, x_rows.reshape(NUM_SEQ, SEQ_LEN, MODEL_DIM)).reshape(ROWS_PART, MODEL_DIM)


def expert_tables(expert_ids, slot_ids, gate_vals):
    source = jnp.arange(ROWS_PART)[:, None] // TOKENS_DEV
    sentinel = EXPERTS * SLOTS_EXPERT
    target = jnp.where(slot_ids >= 0, expert_ids * SLOTS_EXPERT + source * CAPACITY + slot_ids, sentinel).reshape(-1)
    token_of = jnp.broadcast_to(jnp.arange(ROWS_PART)[:, None], (ROWS_PART, TOP_K)).reshape(-1)
    inv_tok = jnp.full((sentinel + 1,), ROWS_PART, jnp.int32).at[target].set(token_of)[:sentinel]
    inv_gate = jnp.zeros((sentinel + 1,), jnp.float32).at[target].set(gate_vals.astype(jnp.float32).reshape(-1))[:sentinel]
    return inv_tok.reshape(EXPERTS, SLOTS_EXPERT), inv_gate.reshape(EXPERTS, SLOTS_EXPERT)


def moe_block(h_rows, gain_moe, w_gate, w_up, w_down, inv_tok, inv_gate):
    u_pad = jnp.concatenate([rms_norm(h_rows, gain_moe).astype(jnp.float32), jnp.zeros((1, MODEL_DIM), jnp.float32)], axis=0)

    def expert_step(acc_rows, per_expert):
        tok_idx, gate_col, wg_one, wu_one, wd_one = per_expert
        expert_in = u_pad[tok_idx].astype(jnp.bfloat16)
        z_gate = jnp.dot(expert_in, wg_one.astype(jnp.bfloat16), preferred_element_type=jnp.float32)
        z_up = jnp.dot(expert_in, wu_one.astype(jnp.bfloat16), preferred_element_type=jnp.float32)
        hidden_act = (jax.nn.silu(z_gate) * z_up).astype(jnp.bfloat16)
        expert_out = jnp.dot(hidden_act, wd_one.astype(jnp.bfloat16), preferred_element_type=jnp.float32).astype(jnp.bfloat16)
        return acc_rows.at[tok_idx].add(gate_col[:, None] * expert_out.astype(jnp.float32)), None

    acc_rows, _ = lax.scan(expert_step, jnp.zeros((ROWS_PART + 1, MODEL_DIM), jnp.float32), (inv_tok, inv_gate, w_gate, w_up, w_down))
    return (h_rows.astype(jnp.float32) + acc_rows[:ROWS_PART]).astype(jnp.bfloat16)


def reference(x_a, x_b, dy_b, w_q, w_k, w_v, w_o, gain_attn, gain_moe, w_gate, w_up, w_down, expert_a, slot_a, gate_a, expert_b, slot_b, gate_b):
    def layer(x_rows, wq_in, wk_in, wv_in, wo_in, wg_in, wu_in, wd_in, tables):
        h_rows = attention_block(x_rows, wq_in, wk_in, wv_in, wo_in, gain_attn)
        return moe_block(h_rows, gain_moe, wg_in, wu_in, wd_in, tables[0], tables[1])

    weights = [weight.astype(jnp.float32) for weight in (w_q, w_k, w_v, w_o, w_gate, w_up, w_down)]
    y_a = layer(x_a, weights[0], weights[1], weights[2], weights[3], weights[4], weights[5], weights[6], expert_tables(expert_a, slot_a, gate_a))
    tables_b = expert_tables(expert_b, slot_b, gate_b)
    _, layer_vjp = jax.vjp(lambda x_rows, wq_in, wk_in, wv_in, wo_in, wg_in, wu_in, wd_in: layer(x_rows, wq_in, wk_in, wv_in, wo_in, wg_in, wu_in, wd_in, tables_b), x_b, weights[0], weights[1], weights[2], weights[3], weights[4], weights[5], weights[6])
    grads = layer_vjp(dy_b)
    return (y_a,) + tuple(grads)
```

```python
import functools

import jax
import jax.numpy as jnp
from jax import lax
from jax.experimental import pallas as pl
from jax.experimental.pallas import tpu as pltpu
from jax.sharding import PartitionSpec as P

RMS_EPS = 1e-6
HEAD_DIM = 128
SEQ_MAX = 256
FAR = 1 << 20
BF = jnp.bfloat16
F32 = jnp.float32
VMEM_LIMIT = 60 * 1024 * 1024


def capacity_of(tokens, choices, num_experts):
    return ((3 * tokens * choices // num_experts + 7) // 8) * 8


def mm(lhs, rhs):
    return jnp.dot(lhs, rhs, preferred_element_type=F32)


def mm_nt(lhs, rhs):
    return lax.dot_general(lhs, rhs, (((1,), (1,)), ((), ())), preferred_element_type=F32)


def mm_tn(lhs, rhs):
    return lax.dot_general(lhs, rhs, (((0,), (0,)), ((), ())), preferred_element_type=F32)


def inv_rms_of(rows_f):
    return lax.rsqrt(jnp.mean(rows_f * rows_f, axis=-1, keepdims=True) + RMS_EPS)


def norm_rows(rows_f, gain_row):
    return (rows_f * inv_rms_of(rows_f) * gain_row).astype(BF)


def norm_back(rows_f, gain_row, d_normed):
    inv = inv_rms_of(rows_f)
    scaled = d_normed.astype(F32) * gain_row
    dot_mean = jnp.mean(scaled * rows_f, axis=-1, keepdims=True)
    return (scaled * inv - rows_f * (inv * inv * inv * dot_mean)).astype(BF)


def pack_rows(pos_row, src_ref, dst_ref, chunk):
    tokens = pos_row.shape[1]

    def body(c, carry):
        base = pl.multiple_of(c * chunk, chunk)
        want = base + lax.broadcasted_iota(jnp.int32, (chunk, tokens), 0)
        onehot = jnp.where(want == pos_row, 1.0, 0.0).astype(BF)
        dst_ref[pl.ds(base, chunk), :] = mm(onehot, src_ref[...]).astype(BF)
        return carry

    lax.fori_loop(0, dst_ref.shape[0] // chunk, body, 0)


def unpack_rows(pos_col, num_experts, back_ref):
    seg = back_ref.shape[0] // num_experts
    total = jnp.zeros((pos_col.shape[0], back_ref.shape[1]), F32)
    for e in range(num_experts):
        want = e * seg + lax.broadcasted_iota(jnp.int32, (pos_col.shape[0], seg), 1)
        total += mm(jnp.where(want == pos_col, 1.0, 0.0).astype(BF), back_ref[pl.ds(e * seg, seg), :])
    return total


def route_one(e_ref, s_ref, pos_ref, num_experts, seg):
    tokens = e_ref.shape[1]
    expert = e_ref[...]
    kept = s_ref[...] >= 0
    lane_expert = lax.broadcasted_iota(jnp.int32, (num_experts, tokens), 0)
    onehot_f = jnp.where((lane_expert == expert) & kept, 1.0, 0.0)
    onehot = onehot_f.astype(BF)
    before = lax.broadcasted_iota(jnp.int32, (tokens, tokens), 0) < lax.broadcasted_iota(jnp.int32, (tokens, tokens), 1)
    rank = mm(onehot, jnp.where(before, 1.0, 0.0).astype(BF))
    pos = expert * seg + jnp.sum(onehot_f * rank, axis=0, keepdims=True).astype(jnp.int32)
    pos = jnp.where(kept, pos, FAR)
    pos_ref[...] = pos
    return pos


def route_kernel(num_experts, ea_ref, sa_ref, eb_ref, sb_ref, gate_ref, dy_ref, pos_a_ref, pos_b_ref, d_pack_ref, scaled):
    seg = d_pack_ref.shape[0] // num_experts
    route_one(ea_ref, sa_ref, pos_a_ref, num_experts, seg)
    pos_b = route_one(eb_ref, sb_ref, pos_b_ref, num_experts, seg)
    scaled[...] = (dy_ref[...].astype(F32) * gate_ref[...].astype(F32)).astype(BF)
    pack_rows(pos_b, scaled, d_pack_ref, seg)


def route(expert_a, slot_a, expert_b, slot_b, gate_b, dy_b, num_experts, seg):
    tokens, hidden = dy_b.shape
    row = jax.ShapeDtypeStruct((1, tokens), jnp.int32)
    return pl.pallas_call(
        functools.partial(route_kernel, num_experts),
        out_shape=(row, row, jax.ShapeDtypeStruct((num_experts * seg, hidden), BF)),
        scratch_shapes=[pltpu.VMEM((tokens, hidden), BF)],
        compiler_params=pltpu.CompilerParams(vmem_limit_bytes=VMEM_LIMIT),
        cost_estimate=pl.CostEstimate(flops=4 * tokens * tokens * hidden, bytes_accessed=2 * 2 * tokens * hidden, transcendentals=0),
        name='route',
    )(expert_a.reshape(1, tokens), slot_a.reshape(1, tokens), expert_b.reshape(1, tokens), slot_b.reshape(1, tokens), gate_b, dy_b)


def softmax_head(q_head, k_head, causal):
    scores = jnp.where(causal, mm_nt(q_head, k_head) * HEAD_DIM ** -0.5, -1e30)
    expd = jnp.exp(scores - jnp.max(scores, axis=-1, keepdims=True))
    return expd * (1.0 / jnp.sum(expd, axis=-1, keepdims=True))


def causal_mask(seq_len):
    return lax.broadcasted_iota(jnp.int32, (seq_len, seq_len), 0) >= lax.broadcasted_iota(jnp.int32, (seq_len, seq_len), 1)


def attn_kernel(chunk, x_ref, wq_ref, wk_ref, wv_ref, wo_ref, ga_ref, gm_ref, pos_ref, h_ref, pack_ref, *rest):
    q_ref, k_ref, v_ref, mixed_ref, u_all = rest
    seq_len, hidden = x_ref.shape
    x_f = x_ref[...].astype(F32)
    normed = norm_rows(x_f, ga_ref[...])
    q_ref[...] = mm(normed, wq_ref[...]).astype(BF)
    k_ref[...] = mm(normed, wk_ref[...]).astype(BF)
    v_ref[...] = mm(normed, wv_ref[...]).astype(BF)
    causal = causal_mask(seq_len)
    for head in range(hidden // HEAD_DIM):
        cols = pl.ds(head * HEAD_DIM, HEAD_DIM)
        probs = softmax_head(q_ref[:, cols], k_ref[:, cols], causal).astype(BF)
        mixed_ref[:, cols] = mm(probs, v_ref[:, cols]).astype(BF)
    h_rows = (x_f + mm(mixed_ref[...], wo_ref[...])).astype(BF)
    h_ref[...] = h_rows
    step = pl.program_id(0)
    u_all[pl.ds(pl.multiple_of(step * seq_len, seq_len), seq_len), :] = norm_rows(h_rows.astype(F32), gm_ref[...])

    @pl.when(step == pl.num_programs(0) - 1)
    def _():
        pack_rows(pos_ref[...], u_all, pack_ref, chunk)


def attn_forward(x_rows, w_q, w_k, w_v, w_o, gain_attn, gain_moe, pos_row, keep, num_experts, seg):
    tokens, hidden = x_rows.shape
    seq_len = min(tokens, SEQ_MAX)
    seqs = tokens // seq_len
    rows = pl.BlockSpec((seq_len, hidden), lambda i: (i, 0))
    whole = pl.BlockSpec((hidden, hidden), lambda i: (0, 0))
    gain = pl.BlockSpec((1, hidden), lambda i: (0, 0))
    full = jax.ShapeDtypeStruct((tokens, hidden), BF)
    out_shape = [full, jax.ShapeDtypeStruct((num_experts * seg, hidden), BF)]
    out_specs = [rows, pl.BlockSpec((num_experts * seg, hidden), lambda i: (0, 0))]
    scratch = [pltpu.VMEM((tokens, hidden), BF)]
    if keep:
        out_shape += [full] * 4
        out_specs += [rows] * 4
    else:
        scratch = [pltpu.VMEM((seq_len, hidden), BF)] * 4 + scratch
    return pl.pallas_call(
        functools.partial(attn_kernel, seg),
        grid=(seqs,),
        in_specs=[rows, whole, whole, whole, whole, gain, gain, pl.BlockSpec((1, tokens), lambda i: (0, 0))],
        out_specs=out_specs,
        out_shape=out_shape,
        scratch_shapes=scratch,
        compiler_params=pltpu.CompilerParams(vmem_limit_bytes=VMEM_LIMIT, dimension_semantics=('arbitrary',)),
        cost_estimate=pl.CostEstimate(flops=14 * tokens * hidden * hidden, bytes_accessed=20 * tokens * hidden, transcendentals=tokens * seq_len * 6),
        name='attn_fwd_keep' if keep else 'attn_fwd',
    )(x_rows, w_q, w_k, w_v, w_o, gain_attn[None, :], gain_moe[None, :], pos_row)


def weight_specs(hidden, ff):
    up = pl.BlockSpec((hidden, ff), lambda i, n, ids: (0, 0), pipeline_mode=pl.Buffered(1))
    down = pl.BlockSpec((ff, hidden), lambda i, n, ids: (0, 0), pipeline_mode=pl.Buffered(1))
    return [up, up, down]


def pick_specs(half, hidden):
    def picked(part):
        return pl.BlockSpec((half, hidden), lambda i, n, ids: (ids[jnp.minimum(2 * i + part, jnp.maximum(n[0] - 1, 0))], 0))

    return [picked(0), picked(1)]


def join_pair(first_ref, second_ref, both):
    second = second_ref[...]
    return jnp.concatenate([first_ref[...], jnp.where(both, second, jnp.zeros_like(second))], axis=0)


def pair_loop(n_ref, ids_ref, buf, out_ref, sem, half, compute):
    step = pl.program_id(0)
    steps = pl.num_programs(0)

    def copies(at):
        slot = lax.rem(at, 2)
        return [
            pltpu.make_async_copy(
                buf.at[slot, pl.ds(part * half, half), :],
                out_ref.at[pl.ds(pl.multiple_of(ids_ref[2 * at + part] * half, half), half), :],
                sem.at[slot, part],
            )
            for part in range(2)
        ]

    def drain(at):
        for copy in copies(at):
            copy.wait()

    @pl.when(step >= 2)
    def _():
        drain(step - 2)

    dst = buf.at[lax.rem(step, 2)]

    @pl.when(2 * step < n_ref[0])
    def _():
        compute(2 * step + 1 < n_ref[0], dst)

    @pl.when(2 * step >= n_ref[0])
    def _():
        dst[...] = jnp.zeros_like(dst)

    for copy in copies(step):
        copy.start()

    @pl.when(step == steps - 1)
    def _():
        drain(step - 1)
        drain(step)


def ffn_fwd_kernel(half, chunk, n_ref, ids_ref, u0_ref, u1_ref, wg_ref, wu_ref, wd_ref, o_ref, acc, buf, sem):
    def compute(both, dst):
        u_rows = join_pair(u0_ref, u1_ref, both)
        acc[...] = jnp.zeros_like(acc)

        def body(c, carry):
            cols = pl.ds(pl.multiple_of(c * chunk, chunk), chunk)
            z_gate = mm(u_rows, wg_ref[:, cols])
            z_up = mm(u_rows, wu_ref[:, cols])
            act = (z_gate * jax.nn.sigmoid(z_gate) * z_up).astype(BF)
            acc[...] += mm(act, wd_ref[cols, :])
            return carry

        lax.fori_loop(0, wg_ref.shape[1] // chunk, body, 0)
        dst[...] = acc[...].astype(BF)

    pair_loop(n_ref, ids_ref, buf, o_ref, sem, half, compute)


def pair_scratch(half, hidden):
    return [pltpu.VMEM((2 * half, hidden), F32), pltpu.VMEM((2, 2 * half, hidden), BF), pltpu.SemaphoreType.DMA((2, 2))]


def ffn_forward(n_blocks, ids, u_rows, w_gate, w_up, w_down, half=128, chunk=512):
    rows, hidden = u_rows.shape
    ff = w_gate.shape[1]
    return pl.pallas_call(
        functools.partial(ffn_fwd_kernel, half, chunk),
        grid_spec=pltpu.PrefetchScalarGridSpec(
            num_scalar_prefetch=2,
            grid=(rows // (2 * half),),
            in_specs=pick_specs(half, hidden) + weight_specs(hidden, ff),
            out_specs=pl.BlockSpec(memory_space=pl.ANY),
            scratch_shapes=pair_scratch(half, hidden),
        ),
        out_shape=jax.ShapeDtypeStruct((rows, hidden), BF),
        compiler_params=pltpu.CompilerParams(vmem_limit_bytes=VMEM_LIMIT, dimension_semantics=('arbitrary',)),
        cost_estimate=pl.CostEstimate(flops=3 * rows * hidden * ff, bytes_accessed=6 * hidden * ff, transcendentals=0),
        name='ffn_fwd',
    )(n_blocks, ids, u_rows, u_rows, w_gate, w_up, w_down)


def ffn_bwd_kernel(half, chunk, n_ref, ids_ref, u0_ref, u1_ref, d0_ref, d1_ref, wg_ref, wu_ref, wd_ref, din_ref, uc_ref, dc_ref, act_ref, dzg_ref, dzu_ref, acc, buf, sem):
    def compute(both, dst):
        u_rows = join_pair(u0_ref, u1_ref, both)
        d_out = join_pair(d0_ref, d1_ref, both)
        uc_ref[...] = u_rows
        dc_ref[...] = d_out
        acc[...] = jnp.zeros_like(acc)

        def body(c, carry):
            cols = pl.ds(pl.multiple_of(c * chunk, chunk), chunk)
            z_gate = mm(u_rows, wg_ref[:, cols])
            z_up = mm(u_rows, wu_ref[:, cols])
            d_act = mm_nt(d_out, wd_ref[cols, :]).astype(BF).astype(F32)
            sig = jax.nn.sigmoid(z_gate)
            silu = z_gate * sig
            act_ref[:, cols] = (silu * z_up).astype(BF)
            d_zg = (d_act * z_up * sig * (1.0 + z_gate * (1.0 - sig))).astype(BF)
            d_zu = (d_act * silu).astype(BF)
            dzg_ref[:, cols] = d_zg
            dzu_ref[:, cols] = d_zu
            acc[...] += mm_nt(d_zg, wg_ref[:, cols]) + mm_nt(d_zu, wu_ref[:, cols])
            return carry

        lax.fori_loop(0, wg_ref.shape[1] // chunk, body, 0)
        dst[...] = acc[...].astype(BF)

    pair_loop(n_ref, ids_ref, buf, din_ref, sem, half, compute)


def step_index(n_ref, i):
    return jnp.minimum(i, jnp.maximum((n_ref[0] + 1) // 2 - 1, 0))


def ffn_backward(n_blocks, ids, u_rows, d_out, w_gate, w_up, w_down, half=128, chunk=512):
    rows, hidden = u_rows.shape
    ff = w_gate.shape[1]
    row_spec = pl.BlockSpec((2 * half, hidden), lambda i, n, ids: (step_index(n, i), 0))
    wide_spec = pl.BlockSpec((2 * half, ff), lambda i, n, ids: (step_index(n, i), 0))
    thin, wide = jax.ShapeDtypeStruct((rows, hidden), BF), jax.ShapeDtypeStruct((rows, ff), BF)
    return pl.pallas_call(
        functools.partial(ffn_bwd_kernel, half, chunk),
        grid_spec=pltpu.PrefetchScalarGridSpec(
            num_scalar_prefetch=2,
            grid=(rows // (2 * half),),
            in_specs=pick_specs(half, hidden) + pick_specs(half, hidden) + weight_specs(hidden, ff),
            out_specs=[pl.BlockSpec(memory_space=pl.ANY), row_spec, row_spec, wide_spec, wide_spec, wide_spec],
            scratch_shapes=pair_scratch(half, hidden),
        ),
        out_shape=(thin, thin, thin, wide, wide, wide),
        compiler_params=pltpu.CompilerParams(vmem_limit_bytes=VMEM_LIMIT, dimension_semantics=('arbitrary',)),
        cost_estimate=pl.CostEstimate(flops=6 * rows * hidden * ff, bytes_accessed=6 * hidden * ff + 3 * rows * ff, transcendentals=0),
        name='ffn_bwd',
    )(n_blocks, ids, u_rows, u_rows, d_out, d_out, w_gate, w_up, w_down)


def ffn_grad_kernel(n_ref, u_ref, d_ref, act_ref, dzg_ref, dzu_ref, dwg_ref, dwu_ref, dwd_ref):
    step = pl.program_id(1)

    @pl.when(step == 0)
    def _():
        dwg_ref[...] = jnp.zeros_like(dwg_ref)
        dwu_ref[...] = jnp.zeros_like(dwu_ref)
        dwd_ref[...] = jnp.zeros_like(dwd_ref)

    @pl.when(2 * step < n_ref[0])
    def _():
        dwg_ref[...] += mm_tn(u_ref[...], dzg_ref[...])
        dwu_ref[...] += mm_tn(u_ref[...], dzu_ref[...])
        dwd_ref[...] += mm_tn(act_ref[...], d_ref[...])


def ffn_grads(n_blocks, u_rows, d_out, act, d_zg, d_zu, block=256, chunk=1024):
    rows, hidden = u_rows.shape
    ff = act.shape[1]
    row_spec = pl.BlockSpec((block, hidden), lambda j, i, n: (step_index(n, i), 0))
    wide_spec = pl.BlockSpec((block, chunk), lambda j, i, n: (step_index(n, i), j))
    up_spec = pl.BlockSpec((hidden, chunk), lambda j, i, n: (0, j))
    down_spec = pl.BlockSpec((chunk, hidden), lambda j, i, n: (j, 0))
    return pl.pallas_call(
        ffn_grad_kernel,
        grid_spec=pltpu.PrefetchScalarGridSpec(
            num_scalar_prefetch=1,
            grid=(ff // chunk, rows // block),
            in_specs=[row_spec, row_spec, wide_spec, wide_spec, wide_spec],
            out_specs=[up_spec, up_spec, down_spec],
        ),
        out_shape=(jax.ShapeDtypeStruct((hidden, ff), F32), jax.ShapeDtypeStruct((hidden, ff), F32), jax.ShapeDtypeStruct((ff, hidden), F32)),
        compiler_params=pltpu.CompilerParams(vmem_limit_bytes=VMEM_LIMIT, dimension_semantics=('arbitrary', 'arbitrary')),
        cost_estimate=pl.CostEstimate(flops=3 * rows * hidden * ff, bytes_accessed=12 * hidden * ff + 3 * rows * ff, transcendentals=0),
        name='ffn_grads',
    )(n_blocks, u_rows, d_out, act, d_zg, d_zu)


def attn_bwd_kernel(num_experts, x_ref, h_ref, dy_ref, q_ref, k_ref, v_ref, mixed_ref, back_ref, pos_ref, wq_ref, wk_ref, wv_ref, wo_ref, ga_ref, gm_ref, dx_ref, dw_ref, dq, dk, dv, dmix):
    seq_len, hidden = x_ref.shape
    d_u = unpack_rows(pos_ref[...], num_experts, back_ref).astype(BF)
    d_h = (dy_ref[...].astype(F32) + norm_back(h_ref[...].astype(F32), gm_ref[...], d_u).astype(F32)).astype(BF)
    dmix[...] = mm_nt(d_h, wo_ref[...]).astype(BF)
    causal = causal_mask(seq_len)
    for head in range(hidden // HEAD_DIM):
        cols = pl.ds(head * HEAD_DIM, HEAD_DIM)
        q_head, k_head, v_head, d_mixed = q_ref[:, cols], k_ref[:, cols], v_ref[:, cols], dmix[:, cols]
        probs = softmax_head(q_head, k_head, causal)
        d_probs = mm_nt(d_mixed, v_head)
        dv[:, cols] = mm_tn(probs.astype(BF), d_mixed).astype(BF)
        d_scores = (probs * (d_probs - jnp.sum(d_probs * probs, axis=-1, keepdims=True)) * HEAD_DIM ** -0.5).astype(BF)
        dq[:, cols] = mm(d_scores, k_head).astype(BF)
        dk[:, cols] = mm_tn(d_scores, q_head).astype(BF)
    x_f = x_ref[...].astype(F32)
    normed = norm_rows(x_f, ga_ref[...])

    @pl.when(pl.program_id(0) == 0)
    def _():
        dw_ref[...] = jnp.zeros_like(dw_ref)

    normed_t = normed.T
    dw_ref[0] += mm(normed_t, dq[...])
    dw_ref[1] += mm(normed_t, dk[...])
    dw_ref[2] += mm(normed_t, dv[...])
    dw_ref[3] += mm_tn(mixed_ref[...], d_h)
    d_normed = (mm_nt(dq[...], wq_ref[...]) + mm_nt(dk[...], wk_ref[...]) + mm_nt(dv[...], wv_ref[...])).astype(BF)
    dx_ref[...] = (d_h.astype(F32) + norm_back(x_f, ga_ref[...], d_normed).astype(F32)).astype(BF)


def attn_backward(num_experts, x_rows, h_rows, dy_rows, saved, back, pos_col, w_q, w_k, w_v, w_o, gain_attn, gain_moe):
    tokens, hidden = x_rows.shape
    seq_len = min(tokens, SEQ_MAX)
    rows = pl.BlockSpec((seq_len, hidden), lambda i: (i, 0))
    whole = pl.BlockSpec((hidden, hidden), lambda i: (0, 0))
    gain = pl.BlockSpec((1, hidden), lambda i: (0, 0))
    return pl.pallas_call(
        functools.partial(attn_bwd_kernel, num_experts),
        grid=(tokens // seq_len,),
        in_specs=[rows] * 7 + [pl.BlockSpec(back.shape, lambda i: (0, 0)), pl.BlockSpec((seq_len, 1), lambda i: (i, 0))] + [whole] * 4 + [gain] * 2,
        out_specs=[rows, pl.BlockSpec((4, hidden, hidden), lambda i: (0, 0, 0))],
        out_shape=(jax.ShapeDtypeStruct((tokens, hidden), BF), jax.ShapeDtypeStruct((4, hidden, hidden), F32)),
        scratch_shapes=[pltpu.VMEM((seq_len, hidden), BF)] * 4,
        compiler_params=pltpu.CompilerParams(vmem_limit_bytes=VMEM_LIMIT, dimension_semantics=('arbitrary',)),
        cost_estimate=pl.CostEstimate(flops=26 * tokens * hidden * hidden, bytes_accessed=40 * tokens * hidden, transcendentals=tokens * seq_len * 6),
        name='attn_bwd',
    )(x_rows, h_rows, dy_rows, *saved, back, pos_col, w_q, w_k, w_v, w_o, gain_attn[None, :], gain_moe[None, :])


def combine_kernel(num_experts, h_ref, back_ref, pos_ref, gate_ref, y_ref):
    picked = unpack_rows(pos_ref[...], num_experts, back_ref)
    y_ref[...] = (h_ref[...].astype(F32) + gate_ref[...].astype(F32) * picked).astype(BF)


def combine(num_experts, h_rows, back, pos_col, gate_col):
    tokens, hidden = h_rows.shape
    block = min(tokens, 256)
    rows = pl.BlockSpec((block, hidden), lambda i: (i, 0))
    one = pl.BlockSpec((block, 1), lambda i: (i, 0))
    return pl.pallas_call(
        functools.partial(combine_kernel, num_experts),
        grid=(tokens // block,),
        in_specs=[rows, pl.BlockSpec(back.shape, lambda i: (0, 0)), one, one],
        out_specs=rows,
        out_shape=jax.ShapeDtypeStruct((tokens, hidden), BF),
        compiler_params=pltpu.CompilerParams(vmem_limit_bytes=VMEM_LIMIT, dimension_semantics=('arbitrary',)),
        cost_estimate=pl.CostEstimate(flops=2 * tokens * tokens * hidden, bytes_accessed=6 * tokens * hidden, transcendentals=0),
        name='combine',
    )(h_rows, back, pos_col, gate_col)


def active_blocks(rows, half):
    blocks = rows.shape[0] // half
    flags = jnp.any(rows.reshape(blocks, half, rows.shape[1]) != 0, axis=(1, 2)).astype(jnp.int32)
    earlier = jnp.arange(blocks)[:, None] < jnp.arange(blocks)[None, :]
    total = jnp.sum(flags)
    rank_on = jnp.sum(jnp.where(earlier, flags[:, None], 0), axis=0)
    rank_off = total + jnp.sum(jnp.where(earlier, 1 - flags[:, None], 0), axis=0)
    rank = jnp.where(flags > 0, rank_on, rank_off)
    ids = jnp.sum(jnp.where(rank[None, :] == jnp.arange(blocks)[:, None], jnp.arange(blocks)[None, :], 0), axis=1)
    return total.astype(jnp.int32).reshape(1), ids.astype(jnp.int32)


CHUNK = 64
LAG_TOTAL = 3
LAG_FORWARD = 6


def reduce_kernel(x_ref, *rest):
    outs, (prt, acc, from_end, from_mid, tot, s_prt, r_prt, s_up, r_up, s_mid, r_mid, s_end, s_fwd, s_share, r_tot, r_share, s_out) = rest[:4], rest[4:]
    me = lax.axis_index('ep')
    core, z = lax.rem(me, 2), me // 2
    is_mid = (z == 1) | (z == 2)
    is_end = jnp.logical_not(is_mid)
    side = z // 2
    half = acc.shape[0]
    steps = half // CHUNK
    partner = 2 * z + 1 - core
    mate = 2 * (2 * side + 1 - lax.rem(z, 2)) + core
    across = 2 * (3 - z) + core

    def send(src, dst, send_sem, recv_sem, to):
        return pltpu.make_async_remote_copy(src_ref=src, dst_ref=dst, send_sem=send_sem, recv_sem=recv_sem, device_id={'ep': to}, device_id_type=pl.DeviceIdType.MESH)

    def rows(k):
        return pl.ds(pl.multiple_of(k * CHUNK, CHUNK), CHUNK)

    def mine(k):
        return pl.ds(pl.multiple_of(core * half + k * CHUNK, CHUNK), CHUNK)

    def theirs(k):
        return pl.ds(pl.multiple_of((1 - core) * half + k * CHUNK, CHUNK), CHUNK)

    def c_prt(k):
        return send(x_ref.at[theirs(k), :], prt.at[rows(k), :], s_prt.at[k], r_prt.at[k], partner)

    def c_up(k):
        return send(acc.at[rows(k), :], from_end.at[rows(k), :], s_up.at[k], r_up.at[k], mate)

    def c_mid(k):
        return send(acc.at[rows(k), :], from_mid.at[rows(k), :], s_mid.at[k], r_mid.at[k], across)

    def c_end(k):
        return send(tot.at[mine(k), :], tot.at[mine(k), :], s_end.at[k], r_tot.at[k], mate)

    def c_fwd(k):
        return send(tot.at[mine(k), :], tot.at[mine(k), :], s_fwd.at[k], r_tot.at[k], across)

    def c_share(k):
        return send(tot.at[mine(k), :], tot.at[mine(k), :], s_share.at[k], r_share.at[k], partner)

    barrier = pltpu.get_barrier_semaphore()
    for peer in (partner, mate):
        pl.semaphore_signal(barrier, inc=1, device_id={'ep': peer}, device_id_type=pl.DeviceIdType.MESH)

    @pl.when(is_mid)
    def _():
        pl.semaphore_signal(barrier, inc=1, device_id={'ep': across}, device_id_type=pl.DeviceIdType.MESH)
        pl.semaphore_wait(barrier, 3)

    @pl.when(is_end)
    def _():
        pl.semaphore_wait(barrier, 2)

    def begin(k, carry):
        c_prt(k).start()
        return carry

    lax.fori_loop(0, steps, begin, 0)

    def chip_sum(k):
        c_prt(k).wait_recv()
        acc[rows(k), :] = x_ref[mine(k), :] + prt[rows(k), :]

    @pl.when(is_end)
    def _():
        def up(k, carry):
            chip_sum(k)
            c_up(k).start()
            return carry

        lax.fori_loop(0, steps, up, 0)

        def take(k, carry):
            c_end(k).wait_recv()
            c_share(k).start()
            return carry

        lax.fori_loop(0, steps, take, 0)

    @pl.when(is_mid)
    def _():
        def run(t, carry):
            @pl.when(t < steps)
            def _():
                chip_sum(t)
                c_up(t).wait_recv()
                acc[rows(t), :] += from_end[rows(t), :]

                @pl.when(lax.rem(t, 2) != side)
                def _():
                    c_mid(t).start()

            j = t - LAG_TOTAL

            @pl.when((j >= 0) & (j < steps) & (lax.rem(j + 2, 2) == side))
            def _():
                c_mid(j).wait_recv()
                tot[mine(j), :] = acc[rows(j), :] + from_mid[rows(j), :]
                c_fwd(j).start()
                c_end(j).start()
                c_share(j).start()

            f = t - LAG_FORWARD

            @pl.when((f >= 0) & (lax.rem(f + 6, 2) != side))
            def _():
                c_fwd(f).wait_recv()
                c_end(f).start()
                c_share(f).start()

            return carry

        lax.fori_loop(0, steps + LAG_FORWARD, run, 0)

    def finish(k, carry):
        c_share(k).wait_recv()
        c_prt(k).wait_send()
        c_share(k).wait_send()

        @pl.when(is_end)
        def _():
            c_up(k).wait_send()

        @pl.when(is_mid)
        def _():
            c_end(k).wait_send()

            @pl.when(lax.rem(k, 2) != side)
            def _():
                c_mid(k).wait_send()

            @pl.when(lax.rem(k, 2) == side)
            def _():
                c_fwd(k).wait_send()

        return carry

    lax.fori_loop(0, steps, finish, 0)
    size = outs[0].shape[0]
    flushes = [pltpu.make_async_copy(tot.at[pl.ds(i * size, size), :], out, s_out.at[i]) for i, out in enumerate(outs)]
    for flush in flushes:
        flush.start()
    for flush in flushes:
        flush.wait()


def group_sum(stacked):
    count, size, hidden = stacked.shape
    total = count * size
    half = total // 2
    steps = half // CHUNK
    dma = pltpu.SemaphoreType.DMA((steps,))
    return pl.pallas_call(
        reduce_kernel,
        in_specs=[pl.BlockSpec(memory_space=pltpu.VMEM)],
        out_specs=[pl.BlockSpec(memory_space=pl.ANY)] * count,
        out_shape=[jax.ShapeDtypeStruct((size, hidden), F32)] * count,
        scratch_shapes=[pltpu.VMEM((half, hidden), F32)] * 4 + [pltpu.VMEM((total, hidden), F32)] + [dma] * 11 + [pltpu.SemaphoreType.DMA((count,))],
        compiler_params=pltpu.CompilerParams(vmem_limit_bytes=VMEM_LIMIT, collective_id=0, has_side_effects=True),
        cost_estimate=pl.CostEstimate(flops=10 ** 11, bytes_accessed=8 * total * hidden, transcendentals=0),
        name='group_sum',
    )(stacked.reshape(total, hidden))


def solution(mesh):
    group_size = mesh.shape['ep']
    row_spec = P(('dp', 'ep'), None)
    rep_two = P(None, None)
    rep_one = P(None)
    expert_spec = P('ep', None, None)
    grad_spec = P('dp', None)
    expert_grad_spec = P(('dp', 'ep'), None, None)

    def device_program(x_a, x_b, dy_b, w_q, w_k, w_v, w_o, gain_attn, gain_moe, w_gate, w_up, w_down, expert_a, slot_a, gate_a, expert_b, slot_b, gate_b):
        tokens, hidden = x_a.shape
        num_experts = group_size
        seg = capacity_of(tokens, 1, num_experts)
        half = seg // 3
        w_gate, w_up, w_down = w_gate[0], w_up[0], w_down[0]

        pos_a, pos_b, d_pack = route(expert_a, slot_a, expert_b, slot_b, gate_b, dy_b, num_experts, seg)
        pos_col_a, pos_col_b = pos_a.reshape(tokens, 1), pos_b.reshape(tokens, 1)

        def move(rows):
            return lax.all_to_all(rows.reshape(group_size, seg, hidden), 'ep', 0, 0, tiled=True).reshape(group_size * seg, hidden)

        d_out_b = move(d_pack)
        h_b, pack_b, *saved_b = attn_forward(x_b, w_q, w_k, w_v, w_o, gain_attn, gain_moe, pos_b, True, num_experts, seg)
        recv_b = move(pack_b)
        h_a, pack_a = attn_forward(x_a, w_q, w_k, w_v, w_o, gain_attn, gain_moe, pos_a, False, num_experts, seg)
        recv_a = move(pack_a)

        n_b, ids_b = active_blocks(recv_b, half)
        d_in_b, u_c, d_c, act_b, d_zg, d_zu = ffn_backward(n_b, ids_b, recv_b, d_out_b, w_gate, w_up, w_down, half)
        d_back = move(d_in_b)
        n_a, ids_a = active_blocks(recv_a, half)
        o_a = ffn_forward(n_a, ids_a, recv_a, w_gate, w_up, w_down, half)
        back_a = move(o_a)
        d_wgate, d_wup, d_wdown = ffn_grads(n_b, u_c, d_c, act_b, d_zg, d_zu, 2 * half)

        d_x, attn_grads = attn_backward(num_experts, x_b, h_b, dy_b, saved_b, d_back, pos_col_b, w_q, w_k, w_v, w_o, gain_attn, gain_moe)
        attn_grads = group_sum(attn_grads)
        y_a = combine(num_experts, h_a, back_a, pos_col_a, gate_a)
        return (y_a, d_x, attn_grads[0], attn_grads[1], attn_grads[2], attn_grads[3], d_wgate[None], d_wup[None], d_wdown[None])

    return jax.shard_map(device_program, mesh=mesh, in_specs=(row_spec, row_spec, row_spec, rep_two, rep_two, rep_two, rep_two, rep_one, rep_one, expert_spec, expert_spec, expert_spec, row_spec, row_spec, row_spec, row_spec, row_spec, row_spec), out_specs=(row_spec, row_spec, grad_spec, grad_spec, grad_spec, grad_spec, expert_grad_spec, expert_grad_spec, expert_grad_spec), check_vma=False)
```

```python
import functools

import jax
import jax.numpy as jnp
from jax import lax
from jax.experimental import pallas as pl
from jax.experimental.pallas import tpu as pltpu
from jax.sharding import PartitionSpec as P

RMS_EPS = 1e-6
HEAD_DIM = 128
SEQ_MAX = 256
FAR = 1 << 20
BF = jnp.bfloat16
F32 = jnp.float32
VMEM_LIMIT = 60 * 1024 * 1024


def capacity_of(tokens, choices, num_experts):
    return ((3 * tokens * choices // num_experts + 7) // 8) * 8


def mm(lhs, rhs):
    return jnp.dot(lhs, rhs, preferred_element_type=F32)


def mm_nt(lhs, rhs):
    return lax.dot_general(lhs, rhs, (((1,), (1,)), ((), ())), preferred_element_type=F32)


def mm_tn(lhs, rhs):
    return lax.dot_general(lhs, rhs, (((0,), (0,)), ((), ())), preferred_element_type=F32)


def inv_rms_of(rows_f):
    return lax.rsqrt(jnp.mean(rows_f * rows_f, axis=-1, keepdims=True) + RMS_EPS)


def norm_rows(rows_f, gain_row):
    return (rows_f * inv_rms_of(rows_f) * gain_row).astype(BF)


def norm_back(rows_f, gain_row, d_normed):
    inv = inv_rms_of(rows_f)
    scaled = d_normed.astype(F32) * gain_row
    dot_mean = jnp.mean(scaled * rows_f, axis=-1, keepdims=True)
    return (scaled * inv - rows_f * (inv * inv * inv * dot_mean)).astype(BF)


def pack_rows(pos_row, src_ref, dst_ref, chunk):
    tokens = pos_row.shape[1]

    def body(c, carry):
        base = pl.multiple_of(c * chunk, chunk)
        want = base + lax.broadcasted_iota(jnp.int32, (chunk, tokens), 0)
        onehot = jnp.where(want == pos_row, 1.0, 0.0).astype(BF)
        dst_ref[pl.ds(base, chunk), :] = mm(onehot, src_ref[...]).astype(BF)
        return carry

    lax.fori_loop(0, dst_ref.shape[0] // chunk, body, 0)


def unpack_rows(pos_col, num_experts, back_ref):
    seg = back_ref.shape[0] // num_experts
    total = jnp.zeros((pos_col.shape[0], back_ref.shape[1]), F32)
    for e in range(num_experts):
        want = e * seg + lax.broadcasted_iota(jnp.int32, (pos_col.shape[0], seg), 1)
        total += mm(jnp.where(want == pos_col, 1.0, 0.0).astype(BF), back_ref[pl.ds(e * seg, seg), :])
    return total


def route_one(e_ref, s_ref, pos_ref, num_experts, seg):
    tokens = e_ref.shape[1]
    expert = e_ref[...]
    kept = s_ref[...] >= 0
    lane_expert = lax.broadcasted_iota(jnp.int32, (num_experts, tokens), 0)
    onehot_f = jnp.where((lane_expert == expert) & kept, 1.0, 0.0)
    onehot = onehot_f.astype(BF)
    before = lax.broadcasted_iota(jnp.int32, (tokens, tokens), 0) < lax.broadcasted_iota(jnp.int32, (tokens, tokens), 1)
    rank = mm(onehot, jnp.where(before, 1.0, 0.0).astype(BF))
    pos = expert * seg + jnp.sum(onehot_f * rank, axis=0, keepdims=True).astype(jnp.int32)
    pos = jnp.where(kept, pos, FAR)
    pos_ref[...] = pos
    return pos


def softmax_head(q_head, k_head, causal):
    scores = jnp.where(causal, mm_nt(q_head, k_head) * HEAD_DIM ** -0.5, -1e30)
    expd = jnp.exp(scores - jnp.max(scores, axis=-1, keepdims=True))
    return expd * (1.0 / jnp.sum(expd, axis=-1, keepdims=True))


def causal_mask(seq_len):
    return lax.broadcasted_iota(jnp.int32, (seq_len, seq_len), 0) >= lax.broadcasted_iota(jnp.int32, (seq_len, seq_len), 1)


def attn_rows(x_ref, w_refs, ga_ref, gm_ref, h_ref, q_ref, k_ref, v_ref, mixed_ref, u_all, seq):
    wq_ref, wk_ref, wv_ref, wo_ref = w_refs
    seq_len, hidden = x_ref.shape
    x_f = x_ref[...].astype(F32)
    normed = norm_rows(x_f, ga_ref[...])
    q_ref[...] = mm(normed, wq_ref[...]).astype(BF)
    k_ref[...] = mm(normed, wk_ref[...]).astype(BF)
    v_ref[...] = mm(normed, wv_ref[...]).astype(BF)
    causal = causal_mask(seq_len)
    for head in range(hidden // HEAD_DIM):
        cols = pl.ds(head * HEAD_DIM, HEAD_DIM)
        probs = softmax_head(q_ref[:, cols], k_ref[:, cols], causal).astype(BF)
        mixed_ref[:, cols] = mm(probs, v_ref[:, cols]).astype(BF)
    h_rows = (x_f + mm(mixed_ref[...], wo_ref[...])).astype(BF)
    h_ref[...] = h_rows
    u_all[pl.ds(pl.multiple_of(seq * seq_len, seq_len), seq_len), :] = norm_rows(h_rows.astype(F32), gm_ref[...])


def head_kernel(group, ea_ref, sa_ref, eb_ref, sb_ref, gate_ref, dy_ref, xa_ref, xb_ref, wq_ref, wk_ref, wv_ref, wo_ref, ga_ref, gm_ref,
                pos_a_ref, pos_b_ref, ha_ref, pack_a_ref, hb_ref, q_ref, k_ref, v_ref, mixed_ref, recv_d_ref, recv_u_ref,
                rows_all, pack_d, pack_u, qa, ka, va, ma, send_d, got_d, send_u, got_u, own):
    step = pl.program_id(0)
    seqs = pl.num_programs(0) // 2
    me = lax.axis_index('ep')
    seg = pack_d.shape[0] // group
    w_refs = (wq_ref, wk_ref, wv_ref, wo_ref)

    def rows_of(index):
        return pl.ds(pl.multiple_of(index * seg, seg), seg)

    def out_copy(packed, landing, send_sem, recv_sem, shift):
        to = lax.rem(me + shift, group)
        return pltpu.make_async_remote_copy(
            src_ref=packed.at[rows_of(to), :], dst_ref=landing.at[rows_of(me), :], send_sem=send_sem.at[shift - 1], recv_sem=recv_sem.at[shift - 1],
            device_id={'ep': to}, device_id_type=pl.DeviceIdType.MESH)

    def own_copy(packed, landing, which):
        return pltpu.make_async_copy(packed.at[rows_of(me), :], landing.at[rows_of(me), :], own.at[which])

    def pack_and_send(pos_row, packed, landing, send_sem, recv_sem, which):
        tokens = pos_row.shape[1]

        def pack_for(to):
            want = to * seg + lax.broadcasted_iota(jnp.int32, (seg, tokens), 0)
            onehot = jnp.where(want == pos_row, 1.0, 0.0).astype(BF)
            packed[rows_of(to), :] = mm(onehot, rows_all[...]).astype(BF)

        def body(shift, carry):
            pack_for(lax.rem(me + shift, group))
            out_copy(packed, landing, send_sem, recv_sem, shift).start()
            return carry

        lax.fori_loop(1, group, body, 0)
        pack_for(me)
        own_copy(packed, landing, which).start()

    def finish(packed, landing, send_sem, recv_sem, which):
        def body(shift, carry):
            copy = out_copy(packed, landing, send_sem, recv_sem, shift)
            copy.wait_recv()
            copy.wait_send()
            return carry

        lax.fori_loop(1, group, body, 0)
        own_copy(packed, landing, which).wait()

    @pl.when(step == 0)
    def _():
        barrier = pltpu.get_barrier_semaphore()

        def greet(shift, carry):
            pl.semaphore_signal(barrier, inc=1, device_id={'ep': lax.rem(me + shift, group)}, device_id_type=pl.DeviceIdType.MESH)
            return carry

        lax.fori_loop(1, group, greet, 0)
        pos_b = route_one(eb_ref, sb_ref, pos_b_ref, group, seg)
        rows_all[...] = (dy_ref[...].astype(F32) * gate_ref[...].astype(F32)).astype(BF)
        pl.semaphore_wait(barrier, group - 1)
        pack_and_send(pos_b, pack_d, recv_d_ref, send_d, got_d, 0)

    @pl.when(step < seqs)
    def _():
        attn_rows(xb_ref, w_refs, ga_ref, gm_ref, hb_ref, q_ref, k_ref, v_ref, mixed_ref, rows_all, step)

    @pl.when(step == seqs - 1)
    def _():
        pack_and_send(pos_b_ref[...], pack_u, recv_u_ref, send_u, got_u, 1)

    @pl.when(step >= seqs)
    def _():
        attn_rows(xa_ref, w_refs, ga_ref, gm_ref, ha_ref, qa, ka, va, ma, rows_all, step - seqs)

    @pl.when(step == 2 * seqs - 1)
    def _():
        pos_a = route_one(ea_ref, sa_ref, pos_a_ref, group, seg)
        pack_rows(pos_a, rows_all, pack_a_ref, seg)
        finish(pack_d, recv_d_ref, send_d, got_d, 0)
        finish(pack_u, recv_u_ref, send_u, got_u, 1)


def head(x_a, x_b, dy_b, gate_b, tables, weights, gain_attn, gain_moe, group, seg):
    tokens, hidden = x_a.shape
    seq_len = min(tokens, SEQ_MAX)
    seqs = tokens // seq_len
    rows_b = pl.BlockSpec((seq_len, hidden), lambda i: (jnp.minimum(i, seqs - 1), 0))
    rows_a = pl.BlockSpec((seq_len, hidden), lambda i: (jnp.maximum(i - seqs, 0), 0))
    once = pl.Buffered(1)

    def fixed(*shape):
        return pl.BlockSpec(shape, lambda i: (0,) * len(shape), pipeline_mode=once)

    row = jax.ShapeDtypeStruct((1, tokens), jnp.int32)
    row_out = pl.BlockSpec((1, tokens), lambda i: (0, 0))
    full = jax.ShapeDtypeStruct((tokens, hidden), BF)
    slots = jax.ShapeDtypeStruct((group * seg, hidden), BF)
    dma = pltpu.SemaphoreType.DMA((group - 1,))
    return pl.pallas_call(
        functools.partial(head_kernel, group),
        grid=(2 * seqs,),
        in_specs=[fixed(1, tokens)] * 4 + [fixed(tokens, 1), fixed(tokens, hidden), rows_a, rows_b] + [fixed(hidden, hidden)] * 4 + [fixed(1, hidden)] * 2,
        out_specs=[row_out, row_out, rows_a, pl.BlockSpec((group * seg, hidden), lambda i: (0, 0))] + [rows_b] * 5 + [pl.BlockSpec(memory_space=pl.ANY)] * 2,
        out_shape=[row, row, full, slots] + [full] * 5 + [slots, slots],
        scratch_shapes=[pltpu.VMEM((tokens, hidden), BF), pltpu.VMEM((group * seg, hidden), BF), pltpu.VMEM((group * seg, hidden), BF)]
        + [pltpu.VMEM((seq_len, hidden), BF)] * 4 + [dma] * 4 + [pltpu.SemaphoreType.DMA((2,))],
        compiler_params=pltpu.CompilerParams(vmem_limit_bytes=VMEM_LIMIT, dimension_semantics=('arbitrary',), collective_id=1, has_side_effects=True),
        cost_estimate=pl.CostEstimate(flops=10 ** 11, bytes_accessed=60 * tokens * hidden, transcendentals=0),
        name='head',
    )(*[table.reshape(1, tokens) for table in tables], gate_b, dy_b, x_a, x_b, *weights, gain_attn[None, :], gain_moe[None, :])


def weight_specs(hidden, ff):
    up = pl.BlockSpec((hidden, ff), lambda i, n, ids: (0, 0), pipeline_mode=pl.Buffered(1))
    down = pl.BlockSpec((ff, hidden), lambda i, n, ids: (0, 0), pipeline_mode=pl.Buffered(1))
    return [up, up, down]


def pick_specs(half, hidden):
    def picked(part):
        return pl.BlockSpec((half, hidden), lambda i, n, ids: (ids[jnp.minimum(2 * i + part, jnp.maximum(n[0] - 1, 0))], 0))

    return [picked(0), picked(1)]


def join_pair(first_ref, second_ref, both):
    second = second_ref[...]
    return jnp.concatenate([first_ref[...], jnp.where(both, second, jnp.zeros_like(second))], axis=0)


def pair_loop(n_ref, ids_ref, buf, out_ref, sem, half, compute):
    step = pl.program_id(0)
    steps = pl.num_programs(0)

    def copies(at):
        slot = lax.rem(at, 2)
        return [
            pltpu.make_async_copy(
                buf.at[slot, pl.ds(part * half, half), :],
                out_ref.at[pl.ds(pl.multiple_of(ids_ref[2 * at + part] * half, half), half), :],
                sem.at[slot, part],
            )
            for part in range(2)
        ]

    def drain(at):
        for copy in copies(at):
            copy.wait()

    @pl.when(step >= 2)
    def _():
        drain(step - 2)

    dst = buf.at[lax.rem(step, 2)]

    @pl.when(2 * step < n_ref[0])
    def _():
        compute(2 * step + 1 < n_ref[0], dst)

    @pl.when(2 * step >= n_ref[0])
    def _():
        dst[...] = jnp.zeros_like(dst)

    for copy in copies(step):
        copy.start()

    @pl.when(step == steps - 1)
    def _():
        drain(step - 1)
        drain(step)


def ffn_fwd_kernel(half, chunk, n_ref, ids_ref, u0_ref, u1_ref, wg_ref, wu_ref, wd_ref, o_ref, acc, buf, sem):
    def compute(both, dst):
        u_rows = join_pair(u0_ref, u1_ref, both)
        acc[...] = jnp.zeros_like(acc)

        def body(c, carry):
            cols = pl.ds(pl.multiple_of(c * chunk, chunk), chunk)
            z_gate = mm(u_rows, wg_ref[:, cols])
            z_up = mm(u_rows, wu_ref[:, cols])
            act = (z_gate * jax.nn.sigmoid(z_gate) * z_up).astype(BF)
            acc[...] += mm(act, wd_ref[cols, :])
            return carry

        lax.fori_loop(0, wg_ref.shape[1] // chunk, body, 0)
        dst[...] = acc[...].astype(BF)

    pair_loop(n_ref, ids_ref, buf, o_ref, sem, half, compute)


def pair_scratch(half, hidden):
    return [pltpu.VMEM((2 * half, hidden), F32), pltpu.VMEM((2, 2 * half, hidden), BF), pltpu.SemaphoreType.DMA((2, 2))]


def ffn_forward(n_blocks, ids, u_rows, w_gate, w_up, w_down, half=128, chunk=512):
    rows, hidden = u_rows.shape
    ff = w_gate.shape[1]
    return pl.pallas_call(
        functools.partial(ffn_fwd_kernel, half, chunk),
        grid_spec=pltpu.PrefetchScalarGridSpec(
            num_scalar_prefetch=2,
            grid=(rows // (2 * half),),
            in_specs=pick_specs(half, hidden) + weight_specs(hidden, ff),
            out_specs=pl.BlockSpec(memory_space=pl.ANY),
            scratch_shapes=pair_scratch(half, hidden),
        ),
        out_shape=jax.ShapeDtypeStruct((rows, hidden), BF),
        compiler_params=pltpu.CompilerParams(vmem_limit_bytes=VMEM_LIMIT, dimension_semantics=('arbitrary',)),
        cost_estimate=pl.CostEstimate(flops=3 * rows * hidden * ff, bytes_accessed=6 * hidden * ff, transcendentals=0),
        name='ffn_fwd',
    )(n_blocks, ids, u_rows, u_rows, w_gate, w_up, w_down)


def ffn_bwd_kernel(half, chunk, n_ref, ids_ref, u0_ref, u1_ref, d0_ref, d1_ref, wg_ref, wu_ref, wd_ref, din_ref, uc_ref, dc_ref, act_ref, dzg_ref, dzu_ref, acc, buf, sem):
    def compute(both, dst):
        u_rows = join_pair(u0_ref, u1_ref, both)
        d_out = join_pair(d0_ref, d1_ref, both)
        uc_ref[...] = u_rows
        dc_ref[...] = d_out
        acc[...] = jnp.zeros_like(acc)

        def body(c, carry):
            cols = pl.ds(pl.multiple_of(c * chunk, chunk), chunk)
            z_gate = mm(u_rows, wg_ref[:, cols])
            z_up = mm(u_rows, wu_ref[:, cols])
            d_act = mm_nt(d_out, wd_ref[cols, :]).astype(BF).astype(F32)
            sig = jax.nn.sigmoid(z_gate)
            silu = z_gate * sig
            act_ref[:, cols] = (silu * z_up).astype(BF)
            d_zg = (d_act * z_up * sig * (1.0 + z_gate * (1.0 - sig))).astype(BF)
            d_zu = (d_act * silu).astype(BF)
            dzg_ref[:, cols] = d_zg
            dzu_ref[:, cols] = d_zu
            acc[...] += mm_nt(d_zg, wg_ref[:, cols]) + mm_nt(d_zu, wu_ref[:, cols])
            return carry

        lax.fori_loop(0, wg_ref.shape[1] // chunk, body, 0)
        dst[...] = acc[...].astype(BF)

    pair_loop(n_ref, ids_ref, buf, din_ref, sem, half, compute)


def step_index(n_ref, i):
    return jnp.minimum(i, jnp.maximum((n_ref[0] + 1) // 2 - 1, 0))


def ffn_backward(n_blocks, ids, u_rows, d_out, w_gate, w_up, w_down, half=128, chunk=512):
    rows, hidden = u_rows.shape
    ff = w_gate.shape[1]
    row_spec = pl.BlockSpec((2 * half, hidden), lambda i, n, ids: (step_index(n, i), 0))
    wide_spec = pl.BlockSpec((2 * half, ff), lambda i, n, ids: (step_index(n, i), 0))
    thin, wide = jax.ShapeDtypeStruct((rows, hidden), BF), jax.ShapeDtypeStruct((rows, ff), BF)
    return pl.pallas_call(
        functools.partial(ffn_bwd_kernel, half, chunk),
        grid_spec=pltpu.PrefetchScalarGridSpec(
            num_scalar_prefetch=2,
            grid=(rows // (2 * half),),
            in_specs=pick_specs(half, hidden) + pick_specs(half, hidden) + weight_specs(hidden, ff),
            out_specs=[pl.BlockSpec(memory_space=pl.ANY), row_spec, row_spec, wide_spec, wide_spec, wide_spec],
            scratch_shapes=pair_scratch(half, hidden),
        ),
        out_shape=(thin, thin, thin, wide, wide, wide),
        compiler_params=pltpu.CompilerParams(vmem_limit_bytes=VMEM_LIMIT, dimension_semantics=('arbitrary',)),
        cost_estimate=pl.CostEstimate(flops=6 * rows * hidden * ff, bytes_accessed=6 * hidden * ff + 3 * rows * ff, transcendentals=0),
        name='ffn_bwd',
    )(n_blocks, ids, u_rows, u_rows, d_out, d_out, w_gate, w_up, w_down)


def ffn_grad_kernel(n_ref, u_ref, d_ref, act_ref, dzg_ref, dzu_ref, dwg_ref, dwu_ref, dwd_ref):
    step = pl.program_id(1)

    @pl.when(step == 0)
    def _():
        dwg_ref[...] = jnp.zeros_like(dwg_ref)
        dwu_ref[...] = jnp.zeros_like(dwu_ref)
        dwd_ref[...] = jnp.zeros_like(dwd_ref)

    @pl.when(2 * step < n_ref[0])
    def _():
        dwg_ref[...] += mm_tn(u_ref[...], dzg_ref[...])
        dwu_ref[...] += mm_tn(u_ref[...], dzu_ref[...])
        dwd_ref[...] += mm_tn(act_ref[...], d_ref[...])


def ffn_grads(n_blocks, u_rows, d_out, act, d_zg, d_zu, block=256, chunk=1024):
    rows, hidden = u_rows.shape
    ff = act.shape[1]
    row_spec = pl.BlockSpec((block, hidden), lambda j, i, n: (step_index(n, i), 0))
    wide_spec = pl.BlockSpec((block, chunk), lambda j, i, n: (step_index(n, i), j))
    up_spec = pl.BlockSpec((hidden, chunk), lambda j, i, n: (0, j))
    down_spec = pl.BlockSpec((chunk, hidden), lambda j, i, n: (j, 0))
    return pl.pallas_call(
        ffn_grad_kernel,
        grid_spec=pltpu.PrefetchScalarGridSpec(
            num_scalar_prefetch=1,
            grid=(ff // chunk, rows // block),
            in_specs=[row_spec, row_spec, wide_spec, wide_spec, wide_spec],
            out_specs=[up_spec, up_spec, down_spec],
        ),
        out_shape=(jax.ShapeDtypeStruct((hidden, ff), F32), jax.ShapeDtypeStruct((hidden, ff), F32), jax.ShapeDtypeStruct((ff, hidden), F32)),
        compiler_params=pltpu.CompilerParams(vmem_limit_bytes=VMEM_LIMIT, dimension_semantics=('arbitrary', 'arbitrary')),
        cost_estimate=pl.CostEstimate(flops=3 * rows * hidden * ff, bytes_accessed=12 * hidden * ff + 3 * rows * ff, transcendentals=0),
        name='ffn_grads',
    )(n_blocks, u_rows, d_out, act, d_zg, d_zu)


def attn_bwd_kernel(num_experts, x_ref, h_ref, dy_ref, q_ref, k_ref, v_ref, mixed_ref, back_ref, pos_ref, wq_ref, wk_ref, wv_ref, wo_ref, ga_ref, gm_ref, dx_ref, dw_ref, dq, dk, dv, dmix):
    seq_len, hidden = x_ref.shape
    d_u = unpack_rows(pos_ref[...], num_experts, back_ref).astype(BF)
    d_h = (dy_ref[...].astype(F32) + norm_back(h_ref[...].astype(F32), gm_ref[...], d_u).astype(F32)).astype(BF)
    dmix[...] = mm_nt(d_h, wo_ref[...]).astype(BF)
    causal = causal_mask(seq_len)
    for head in range(hidden // HEAD_DIM):
        cols = pl.ds(head * HEAD_DIM, HEAD_DIM)
        q_head, k_head, v_head, d_mixed = q_ref[:, cols], k_ref[:, cols], v_ref[:, cols], dmix[:, cols]
        probs = softmax_head(q_head, k_head, causal)
        d_probs = mm_nt(d_mixed, v_head)
        dv[:, cols] = mm_tn(probs.astype(BF), d_mixed).astype(BF)
        d_scores = (probs * (d_probs - jnp.sum(d_probs * probs, axis=-1, keepdims=True)) * HEAD_DIM ** -0.5).astype(BF)
        dq[:, cols] = mm(d_scores, k_head).astype(BF)
        dk[:, cols] = mm_tn(d_scores, q_head).astype(BF)
    x_f = x_ref[...].astype(F32)
    normed = norm_rows(x_f, ga_ref[...])

    @pl.when(pl.program_id(0) == 0)
    def _():
        dw_ref[...] = jnp.zeros_like(dw_ref)

    normed_t = normed.T
    dw_ref[0] += mm(normed_t, dq[...])
    dw_ref[1] += mm(normed_t, dk[...])
    dw_ref[2] += mm(normed_t, dv[...])
    dw_ref[3] += mm_tn(mixed_ref[...], d_h)
    d_normed = (mm_nt(dq[...], wq_ref[...]) + mm_nt(dk[...], wk_ref[...]) + mm_nt(dv[...], wv_ref[...])).astype(BF)
    dx_ref[...] = (d_h.astype(F32) + norm_back(x_f, ga_ref[...], d_normed).astype(F32)).astype(BF)


def attn_backward(num_experts, x_rows, h_rows, dy_rows, saved, back, pos_col, w_q, w_k, w_v, w_o, gain_attn, gain_moe):
    tokens, hidden = x_rows.shape
    seq_len = min(tokens, SEQ_MAX)
    rows = pl.BlockSpec((seq_len, hidden), lambda i: (i, 0))
    whole = pl.BlockSpec((hidden, hidden), lambda i: (0, 0))
    gain = pl.BlockSpec((1, hidden), lambda i: (0, 0))
    return pl.pallas_call(
        functools.partial(attn_bwd_kernel, num_experts),
        grid=(tokens // seq_len,),
        in_specs=[rows] * 7 + [pl.BlockSpec(back.shape, lambda i: (0, 0)), pl.BlockSpec((seq_len, 1), lambda i: (i, 0))] + [whole] * 4 + [gain] * 2,
        out_specs=[rows, pl.BlockSpec((4, hidden, hidden), lambda i: (0, 0, 0))],
        out_shape=(jax.ShapeDtypeStruct((tokens, hidden), BF), jax.ShapeDtypeStruct((4, hidden, hidden), F32)),
        scratch_shapes=[pltpu.VMEM((seq_len, hidden), BF)] * 4,
        compiler_params=pltpu.CompilerParams(vmem_limit_bytes=VMEM_LIMIT, dimension_semantics=('arbitrary',)),
        cost_estimate=pl.CostEstimate(flops=26 * tokens * hidden * hidden, bytes_accessed=40 * tokens * hidden, transcendentals=tokens * seq_len * 6),
        name='attn_bwd',
    )(x_rows, h_rows, dy_rows, *saved, back, pos_col, w_q, w_k, w_v, w_o, gain_attn[None, :], gain_moe[None, :])


def combine_kernel(num_experts, h_ref, back_ref, pos_ref, gate_ref, y_ref):
    picked = unpack_rows(pos_ref[...], num_experts, back_ref)
    y_ref[...] = (h_ref[...].astype(F32) + gate_ref[...].astype(F32) * picked).astype(BF)


def combine(num_experts, h_rows, back, pos_col, gate_col):
    tokens, hidden = h_rows.shape
    block = min(tokens, 256)
    rows = pl.BlockSpec((block, hidden), lambda i: (i, 0))
    one = pl.BlockSpec((block, 1), lambda i: (i, 0))
    return pl.pallas_call(
        functools.partial(combine_kernel, num_experts),
        grid=(tokens // block,),
        in_specs=[rows, pl.BlockSpec(back.shape, lambda i: (0, 0)), one, one],
        out_specs=rows,
        out_shape=jax.ShapeDtypeStruct((tokens, hidden), BF),
        compiler_params=pltpu.CompilerParams(vmem_limit_bytes=VMEM_LIMIT, dimension_semantics=('arbitrary',)),
        cost_estimate=pl.CostEstimate(flops=2 * tokens * tokens * hidden, bytes_accessed=6 * tokens * hidden, transcendentals=0),
        name='combine',
    )(h_rows, back, pos_col, gate_col)


def active_blocks(rows, half):
    blocks = rows.shape[0] // half
    flags = jnp.any(rows.reshape(blocks, half, rows.shape[1]) != 0, axis=(1, 2)).astype(jnp.int32)
    earlier = jnp.arange(blocks)[:, None] < jnp.arange(blocks)[None, :]
    total = jnp.sum(flags)
    rank_on = jnp.sum(jnp.where(earlier, flags[:, None], 0), axis=0)
    rank_off = total + jnp.sum(jnp.where(earlier, 1 - flags[:, None], 0), axis=0)
    rank = jnp.where(flags > 0, rank_on, rank_off)
    ids = jnp.sum(jnp.where(rank[None, :] == jnp.arange(blocks)[:, None], jnp.arange(blocks)[None, :], 0), axis=1)
    return total.astype(jnp.int32).reshape(1), ids.astype(jnp.int32)


CHUNK = 64
LAG_TOTAL = 3
LAG_FORWARD = 6


def reduce_kernel(x_ref, *rest):
    outs, (prt, acc, from_end, from_mid, tot, s_prt, r_prt, s_up, r_up, s_mid, r_mid, s_end, s_fwd, s_share, r_tot, r_share, s_out) = rest[:4], rest[4:]
    me = lax.axis_index('ep')
    core, z = lax.rem(me, 2), me // 2
    is_mid = (z == 1) | (z == 2)
    is_end = jnp.logical_not(is_mid)
    side = z // 2
    half = acc.shape[0]
    steps = half // CHUNK
    partner = 2 * z + 1 - core
    mate = 2 * (2 * side + 1 - lax.rem(z, 2)) + core
    across = 2 * (3 - z) + core

    def send(src, dst, send_sem, recv_sem, to):
        return pltpu.make_async_remote_copy(src_ref=src, dst_ref=dst, send_sem=send_sem, recv_sem=recv_sem, device_id={'ep': to}, device_id_type=pl.DeviceIdType.MESH)

    def rows(k):
        return pl.ds(pl.multiple_of(k * CHUNK, CHUNK), CHUNK)

    def mine(k):
        return pl.ds(pl.multiple_of(core * half + k * CHUNK, CHUNK), CHUNK)

    def theirs(k):
        return pl.ds(pl.multiple_of((1 - core) * half + k * CHUNK, CHUNK), CHUNK)

    def c_prt(k):
        return send(x_ref.at[theirs(k), :], prt.at[rows(k), :], s_prt.at[k], r_prt.at[k], partner)

    def c_up(k):
        return send(acc.at[rows(k), :], from_end.at[rows(k), :], s_up.at[k], r_up.at[k], mate)

    def c_mid(k):
        return send(acc.at[rows(k), :], from_mid.at[rows(k), :], s_mid.at[k], r_mid.at[k], across)

    def c_end(k):
        return send(tot.at[mine(k), :], tot.at[mine(k), :], s_end.at[k], r_tot.at[k], mate)

    def c_fwd(k):
        return send(tot.at[mine(k), :], tot.at[mine(k), :], s_fwd.at[k], r_tot.at[k], across)

    def c_share(k):
        return send(tot.at[mine(k), :], tot.at[mine(k), :], s_share.at[k], r_share.at[k], partner)

    barrier = pltpu.get_barrier_semaphore()
    for peer in (partner, mate):
        pl.semaphore_signal(barrier, inc=1, device_id={'ep': peer}, device_id_type=pl.DeviceIdType.MESH)

    @pl.when(is_mid)
    def _():
        pl.semaphore_signal(barrier, inc=1, device_id={'ep': across}, device_id_type=pl.DeviceIdType.MESH)
        pl.semaphore_wait(barrier, 3)

    @pl.when(is_end)
    def _():
        pl.semaphore_wait(barrier, 2)

    def begin(k, carry):
        c_prt(k).start()
        return carry

    lax.fori_loop(0, steps, begin, 0)

    def chip_sum(k):
        c_prt(k).wait_recv()
        acc[rows(k), :] = x_ref[mine(k), :] + prt[rows(k), :]

    @pl.when(is_end)
    def _():
        def up(k, carry):
            chip_sum(k)
            c_up(k).start()
            return carry

        lax.fori_loop(0, steps, up, 0)

        def take(k, carry):
            c_end(k).wait_recv()
            c_share(k).start()
            return carry

        lax.fori_loop(0, steps, take, 0)

    @pl.when(is_mid)
    def _():
        def run(t, carry):
            @pl.when(t < steps)
            def _():
                chip_sum(t)
                c_up(t).wait_recv()
                acc[rows(t), :] += from_end[rows(t), :]

                @pl.when(lax.rem(t, 2) != side)
                def _():
                    c_mid(t).start()

            j = t - LAG_TOTAL

            @pl.when((j >= 0) & (j < steps) & (lax.rem(j + 2, 2) == side))
            def _():
                c_mid(j).wait_recv()
                tot[mine(j), :] = acc[rows(j), :] + from_mid[rows(j), :]
                c_fwd(j).start()
                c_end(j).start()
                c_share(j).start()

            f = t - LAG_FORWARD

            @pl.when((f >= 0) & (lax.rem(f + 6, 2) != side))
            def _():
                c_fwd(f).wait_recv()
                c_end(f).start()
                c_share(f).start()

            return carry

        lax.fori_loop(0, steps + LAG_FORWARD, run, 0)

    def finish(k, carry):
        c_share(k).wait_recv()
        c_prt(k).wait_send()
        c_share(k).wait_send()

        @pl.when(is_end)
        def _():
            c_up(k).wait_send()

        @pl.when(is_mid)
        def _():
            c_end(k).wait_send()

            @pl.when(lax.rem(k, 2) != side)
            def _():
                c_mid(k).wait_send()

            @pl.when(lax.rem(k, 2) == side)
            def _():
                c_fwd(k).wait_send()

        return carry

    lax.fori_loop(0, steps, finish, 0)
    size = outs[0].shape[0]
    flushes = [pltpu.make_async_copy(tot.at[pl.ds(i * size, size), :], out, s_out.at[i]) for i, out in enumerate(outs)]
    for flush in flushes:
        flush.start()
    for flush in flushes:
        flush.wait()


def group_sum(stacked):
    count, size, hidden = stacked.shape
    total = count * size
    half = total // 2
    steps = half // CHUNK
    dma = pltpu.SemaphoreType.DMA((steps,))
    return pl.pallas_call(
        reduce_kernel,
        in_specs=[pl.BlockSpec(memory_space=pltpu.VMEM)],
        out_specs=[pl.BlockSpec(memory_space=pl.ANY)] * count,
        out_shape=[jax.ShapeDtypeStruct((size, hidden), F32)] * count,
        scratch_shapes=[pltpu.VMEM((half, hidden), F32)] * 4 + [pltpu.VMEM((total, hidden), F32)] + [dma] * 11 + [pltpu.SemaphoreType.DMA((count,))],
        compiler_params=pltpu.CompilerParams(vmem_limit_bytes=VMEM_LIMIT, collective_id=0, has_side_effects=True),
        cost_estimate=pl.CostEstimate(flops=10 ** 11, bytes_accessed=8 * total * hidden, transcendentals=0),
        name='group_sum',
    )(stacked.reshape(total, hidden))


def solution(mesh):
    group_size = mesh.shape['ep']
    row_spec = P(('dp', 'ep'), None)
    rep_two = P(None, None)
    rep_one = P(None)
    expert_spec = P('ep', None, None)
    grad_spec = P('dp', None)
    expert_grad_spec = P(('dp', 'ep'), None, None)

    def device_program(x_a, x_b, dy_b, w_q, w_k, w_v, w_o, gain_attn, gain_moe, w_gate, w_up, w_down, expert_a, slot_a, gate_a, expert_b, slot_b, gate_b):
        tokens, hidden = x_a.shape
        num_experts = group_size
        seg = capacity_of(tokens, 1, num_experts)
        half = seg // 3
        w_gate, w_up, w_down = w_gate[0], w_up[0], w_down[0]

        def move(rows):
            return lax.all_to_all(rows.reshape(group_size, seg, hidden), 'ep', 0, 0, tiled=True).reshape(group_size * seg, hidden)

        tables = (expert_a, slot_a, expert_b, slot_b)
        pos_a, pos_b, h_a, pack_a, h_b, *rest = head(x_a, x_b, dy_b, gate_b, tables, (w_q, w_k, w_v, w_o), gain_attn, gain_moe, group_size, seg)
        *saved_b, d_out_b, recv_b = rest
        pos_col_a, pos_col_b = pos_a.reshape(tokens, 1), pos_b.reshape(tokens, 1)
        recv_a = move(pack_a)
        n_b, ids_b = active_blocks(recv_b, half)
        d_in_b, u_c, d_c, act_b, d_zg, d_zu = ffn_backward(n_b, ids_b, recv_b, d_out_b, w_gate, w_up, w_down, half)
        d_back = move(d_in_b)
        n_a, ids_a = active_blocks(recv_a, half)
        o_a = ffn_forward(n_a, ids_a, recv_a, w_gate, w_up, w_down, half)
        back_a = move(o_a)
        d_wgate, d_wup, d_wdown = ffn_grads(n_b, u_c, d_c, act_b, d_zg, d_zu, 2 * half)

        d_x, attn_grads = attn_backward(num_experts, x_b, h_b, dy_b, saved_b, d_back, pos_col_b, w_q, w_k, w_v, w_o, gain_attn, gain_moe)
        attn_grads = group_sum(attn_grads)
        y_a = combine(num_experts, h_a, back_a, pos_col_a, gate_a)
        return (y_a, d_x, attn_grads[0], attn_grads[1], attn_grads[2], attn_grads[3], d_wgate[None], d_wup[None], d_wdown[None])

    return jax.shard_map(device_program, mesh=mesh, in_specs=(row_spec, row_spec, row_spec, rep_two, rep_two, rep_two, rep_two, rep_one, rep_one, expert_spec, expert_spec, expert_spec, row_spec, row_spec, row_spec, row_spec, row_spec, row_spec), out_specs=(row_spec, row_spec, grad_spec, grad_spec, grad_spec, grad_spec, expert_grad_spec, expert_grad_spec, expert_grad_spec), check_vma=False)
```

```python
import functools

import jax
import jax.numpy as jnp
from jax import lax
from jax.experimental import pallas as pl
from jax.experimental.pallas import tpu as pltpu
from jax.sharding import PartitionSpec as P

RMS_EPS = 1e-6
HEAD_DIM = 128
SEQ_MAX = 256
FAR = 1 << 20
BF = jnp.bfloat16
F32 = jnp.float32
VMEM_LIMIT = 60 * 1024 * 1024


def capacity_of(tokens, choices, num_experts):
    return ((3 * tokens * choices // num_experts + 7) // 8) * 8


def params(dims):
    return pltpu.CompilerParams(vmem_limit_bytes=VMEM_LIMIT, dimension_semantics=('arbitrary',) * dims)


def cost(flops, moved):
    return pl.CostEstimate(flops=flops, bytes_accessed=moved, transcendentals=0)


def one_where(condition):
    return jnp.where(condition, 1.0, 0.0).astype(BF)


def iota(shape, dim):
    return lax.broadcasted_iota(jnp.int32, shape, dim)


def mm(lhs, rhs):
    return jnp.dot(lhs, rhs, preferred_element_type=F32)


def mm_nt(lhs, rhs):
    return lax.dot_general(lhs, rhs, (((1,), (1,)), ((), ())), preferred_element_type=F32)


def mm_tn(lhs, rhs):
    return lax.dot_general(lhs, rhs, (((0,), (0,)), ((), ())), preferred_element_type=F32)


def inv_rms_of(rows_f):
    return lax.rsqrt(jnp.mean(rows_f * rows_f, axis=-1, keepdims=True) + RMS_EPS)


def norm_rows(rows_f, gain_row):
    return (rows_f * inv_rms_of(rows_f) * gain_row).astype(BF)


def norm_back(rows_f, gain_row, d_normed):
    inv = inv_rms_of(rows_f)
    scaled = d_normed.astype(F32) * gain_row
    dot_mean = jnp.mean(scaled * rows_f, axis=-1, keepdims=True)
    return (scaled * inv - rows_f * (inv * inv * inv * dot_mean)).astype(BF)


def pack_rows(pos_row, src_ref, dst_ref, chunk):
    tokens = pos_row.shape[1]

    def body(c, carry):
        base = pl.multiple_of(c * chunk, chunk)
        want = base + iota((chunk, tokens), 0)
        onehot = one_where(want == pos_row)
        dst_ref[pl.ds(base, chunk), :] = mm(onehot, src_ref[:]).astype(BF)
        return carry

    lax.fori_loop(0, dst_ref.shape[0] // chunk, body, 0)


def unpack_rows(pos_col, num_experts, back_ref):
    seg = back_ref.shape[0] // num_experts
    total = jnp.zeros((pos_col.shape[0], back_ref.shape[1]), F32)
    for e in range(num_experts):
        want = e * seg + iota((pos_col.shape[0], seg), 1)
        total += mm(one_where(want == pos_col), back_ref[pl.ds(e * seg, seg), :])
    return total


def route_one(e_ref, s_ref, pos_ref, num_experts, seg):
    tokens = e_ref.shape[1]
    expert = e_ref[:]
    kept = s_ref[:] >= 0
    sub_expert = iota((num_experts, tokens), 0)
    onehot_f = jnp.where((sub_expert == expert) & kept, 1.0, 0.0)
    onehot = onehot_f.astype(BF)
    before = iota((tokens, tokens), 0) < iota((tokens, tokens), 1)
    rank = mm(onehot, one_where(before))
    pos = expert * seg + jnp.sum(onehot_f * rank, axis=0, keepdims=True).astype(jnp.int32)
    pos_ref[:] = jnp.where(kept, pos, FAR)
    return expert, kept, onehot_f, rank


def softmax_head(q_head, k_head, causal):
    scores = jnp.where(causal, mm_nt(q_head, k_head) * HEAD_DIM ** -0.5, -1e30)
    expd = jnp.exp(scores - jnp.max(scores, axis=-1, keepdims=True))
    return expd * (1.0 / jnp.sum(expd, axis=-1, keepdims=True))


def causal_mask(seq_len):
    return iota((seq_len, seq_len), 0) >= iota((seq_len, seq_len), 1)


def attn_rows(x_ref, w_refs, ga_ref, gm_ref, h_ref, q_ref, k_ref, v_ref, mixed_ref, u_all, seq):
    wq_ref, wk_ref, wv_ref, wo_ref = w_refs
    seq_len, hidden = x_ref.shape
    x_f = x_ref[:].astype(F32)
    normed = norm_rows(x_f, ga_ref[:])
    q_ref[:] = mm(normed, wq_ref[:]).astype(BF)
    k_ref[:] = mm(normed, wk_ref[:]).astype(BF)
    v_ref[:] = mm(normed, wv_ref[:]).astype(BF)
    causal = causal_mask(seq_len)
    for head in range(hidden // HEAD_DIM):
        cols = pl.ds(head * HEAD_DIM, HEAD_DIM)
        probs = softmax_head(q_ref[:, cols], k_ref[:, cols], causal).astype(BF)
        mixed_ref[:, cols] = mm(probs, v_ref[:, cols]).astype(BF)
    h_rows = (x_f + mm(mixed_ref[:], wo_ref[:])).astype(BF)
    h_ref[:] = h_rows
    u_all[pl.ds(pl.multiple_of(seq * seq_len, seq_len), seq_len), :] = norm_rows(h_rows.astype(F32), gm_ref[:])


PIECES = 4
SEND_ORDER = (1, 2, 3, 0)


def head_kernel(group, ea_ref, sa_ref, eb_ref, sb_ref, gate_ref, dy_ref, xa_ref, xb_ref, wq_ref, wk_ref, wv_ref, wo_ref, ga_ref, gm_ref,
                pos_a_ref, pos_b_ref, ha_ref, pack_a_ref, hb_ref, q_ref, k_ref, v_ref, mixed_ref, recv_d_ref, recv_u_ref,
                rows_all, pos_cross, meta, meta_in, qa, ka, va, ma, slot_rows, s_meta, r_meta, own, *buffers):
    step = pl.program_id(0)
    seqs = pl.num_programs(0) // 2
    me = lax.axis_index('ep')
    core, chip = lax.rem(me, 2), me // 2
    side = chip // 2
    local = lax.rem(me, 4)
    is_mid = (chip == 1) | (chip == 2)
    is_end = jnp.logical_not(is_mid)
    partner = 2 * chip + 1 - core
    relay = 2 * (2 - side) + core
    end_dev = 2 * (3 * side) + core
    tokens = rows_all.shape[0]
    seg = slot_rows.shape[0]
    piece = tokens // PIECES
    w_refs = (wq_ref, wk_ref, wv_ref, wo_ref)
    tensors = (buffers[:10] + (recv_d_ref, 0), buffers[10:] + (recv_u_ref, 1))

    def remote(src, dst, send_sem, recv_sem, to):
        return pltpu.make_async_remote_copy(src_ref=src, dst_ref=dst, send_sem=send_sem, recv_sem=recv_sem, device_id={'ep': to}, device_id_type=pl.DeviceIdType.MESH)

    def part(index, size):
        return pl.ds(pl.multiple_of(index * size, size), size)

    class Exchange:
        def __init__(self, refs):
            (self.near, self.cross, self.win, self.s_near, self.r_near, self.s_cross, self.r_cross, self.s_end, self.r_end, self.pair, self.recv, self.which) = refs
            self.s_pair, self.r_pair = self.pair.at[0], self.pair.at[1]

        def near_copy(self, shift):
            to = lax.rem(local + shift, 4)
            return remote(self.near.at[part(to, seg), :], self.recv.at[part(me, seg), :], self.s_near.at[shift - 1], self.r_near.at[shift - 1], 4 * side + to)

        def self_copy(self):
            return pltpu.make_async_copy(self.near.at[part(local, seg), :], self.recv.at[part(me, seg), :], own.at[self.which])

        def cross_copy(self, a, j):
            at = part(j, piece)
            return remote(self.cross.at[at, :], self.win.at[2 * a + core, at, :], self.s_cross.at[j], self.r_cross.at[a * PIECES + j], relay)

        def end_copy(self, a, j):
            at = self.win.at[2 * a + core, pl.ds(j * piece, piece), :]
            return remote(at, at, self.s_end.at[a * PIECES + j], self.r_end.at[a * PIECES + j], end_dev)

        def pair_copy(self, a, j, whose):
            at = self.win.at[2 * a + whose, pl.ds(j * piece, piece), :]
            return remote(at, at, self.s_pair.at[a * PIECES + j], self.r_pair.at[a * PIECES + j], partner)

        def pack_and_send(self, pos_row, cross_row):
            def pack_for(row, base, size, dst):
                want = base + iota((size, tokens), 0)
                dst[:] = mm(one_where(want == row), rows_all[:]).astype(BF)

            def cross_body(i, carry):
                j = lax.rem(i + SEND_ORDER[0], PIECES)
                pack_for(cross_row, j * piece, piece, self.cross.at[part(j, piece), :])
                self.cross_copy(chip - 2 * side, j).start()
                return carry

            lax.fori_loop(0, PIECES, cross_body, 0)

            def body(shift, carry):
                to = lax.rem(local + shift, 4)
                pack_for(pos_row, (4 * side + to) * seg, seg, self.near.at[part(to, seg), :])
                self.near_copy(shift).start()
                return carry

            lax.fori_loop(1, 4, body, 0)
            pack_for(pos_row, me * seg, seg, self.near.at[part(local, seg), :])
            self.self_copy().start()

        def forward(self, j):
            @pl.when(is_mid)
            def _():
                for a in range(2):
                    self.cross_copy(a, j).wait_recv()
                    if j > 0:
                        self.end_copy(a, j).start()
                    if j < PIECES - 1:
                        self.pair_copy(a, j, core).start()

            if j > 0:
                @pl.when(is_end)
                def _():
                    for a in range(2):
                        self.end_copy(a, j).wait_recv()
                        self.pair_copy(a, j, core).start()

        def arrived(self):
            for role, pieces in ((is_mid, range(PIECES - 1)), (is_end, range(1, PIECES))):
                @pl.when(role)
                def _(pieces=pieces):
                    for a in range(2):
                        for j in pieces:
                            self.pair_copy(a, j, 1 - core).wait_recv()

        def take(self):
            base = jnp.where(is_mid, 0, piece)

            def body(source, carry):
                first = meta_in[source, pl.ds(me, 1), :][:, :1]
                count = meta_in[source, pl.ds(group + me, 1), :][:, :1]
                window = self.win[source, pl.ds(pl.multiple_of(base, piece), tokens - piece), :]
                slot = iota((seg, tokens - piece), 0)
                lane = base + iota((seg, tokens - piece), 1)
                pick = one_where((lane == first + slot) & (slot < count))
                slot_rows[:] = mm(pick, window).astype(BF)
                flush = pltpu.make_async_copy(slot_rows, self.recv.at[part(4 * (1 - side) + source, seg), :], own.at[self.which])
                flush.start()
                flush.wait()
                return carry

            lax.fori_loop(0, 4, body, 0)

        def finish(self):
            for shift in range(1, 4):
                self.near_copy(shift).wait_recv()
                self.near_copy(shift).wait_send()
            for j in range(PIECES):
                self.cross_copy(chip - 2 * side, j).wait_send()
            for role, pieces in ((is_mid, range(PIECES - 1)), (is_end, range(1, PIECES))):
                @pl.when(role)
                def _(pieces=pieces):
                    for a in range(2):
                        for j in pieces:
                            self.pair_copy(a, j, core).wait_send()

            @pl.when(is_mid)
            def _():
                for a in range(2):
                    for j in range(1, PIECES):
                        self.end_copy(a, j).wait_send()

    exch_d, exch_u = Exchange(tensors[0]), Exchange(tensors[1])

    def meta_copy(shift):
        to = 4 * (1 - side) + lax.rem(local + shift, 4)
        return remote(meta, meta_in.at[local], s_meta.at[shift], r_meta.at[shift], to)

    @pl.when(step == 0)
    def _():
        barrier = pltpu.get_barrier_semaphore()

        def greet(shift, carry):
            pl.semaphore_signal(barrier, inc=1, device_id={'ep': lax.rem(me + shift, group)}, device_id_type=pl.DeviceIdType.MESH)
            return carry

        lax.fori_loop(1, group, greet, 0)
        expert, kept, onehot_f, rank = route_one(eb_ref, sb_ref, pos_b_ref, group, seg)
        row_e = iota((group, group), 0)
        col_e = iota((group, group), 1)
        row_mid = (row_e >= 2) & (row_e < 6)
        same_chip = (row_e // 2) == (col_e // 2)
        reach = jnp.where(same_chip & ((row_mid & (col_e < row_e)) | (jnp.logical_not(row_mid) & (col_e >= row_e))), 1.0, 0.0).astype(BF)
        reached = jnp.sum(mm(reach, onehot_f.astype(BF)), axis=1, keepdims=True)
        one_e = iota((group, 1), 0)
        start = jnp.where((one_e >= 2) & (one_e < 6), reached, tokens - reached)
        count = jnp.sum(onehot_f, axis=1, keepdims=True)
        meta[pl.ds(0, group), :] = jnp.broadcast_to(start.astype(jnp.int32), (group, 128))
        meta[pl.ds(group, group), :] = jnp.broadcast_to(count.astype(jnp.int32), (group, 128))
        at = jnp.sum(onehot_f * (start + rank), axis=0, keepdims=True).astype(jnp.int32)
        pos_cross[:] = jnp.where(kept & ((expert // 4) != side), at, FAR)
        rows_all[:] = (dy_ref[:].astype(F32) * gate_ref[:].astype(F32)).astype(BF)
        pl.semaphore_wait(barrier, group - 1)
        for shift in range(4):
            meta_copy(shift).start()
        exch_d.pack_and_send(pos_b_ref[:], pos_cross[:])

    @pl.when(step < seqs)
    def _():
        attn_rows(xb_ref, w_refs, ga_ref, gm_ref, hb_ref, q_ref, k_ref, v_ref, mixed_ref, rows_all, step)

    @pl.when(step == seqs - 1)
    def _():
        exch_u.pack_and_send(pos_b_ref[:], pos_cross[:])

    for late, j in enumerate(SEND_ORDER):
        @pl.when(step == seqs - 1 + late)
        def _(j=j):
            exch_d.forward(j)

    @pl.when(step >= seqs)
    def _():
        attn_rows(xa_ref, w_refs, ga_ref, gm_ref, ha_ref, qa, ka, va, ma, rows_all, step - seqs)

    @pl.when(step == 2 * seqs - 1)
    def _():
        route_one(ea_ref, sa_ref, pos_a_ref, group, seg)
        pack_rows(pos_a_ref[:], rows_all, pack_a_ref, seg)
        exch_u.forward(SEND_ORDER[0])
        for shift in range(4):
            meta_copy(shift).wait_recv()
            meta_copy(shift).wait_send()
        exch_d.self_copy().wait()
        exch_u.self_copy().wait()
        exch_d.arrived()
        exch_d.take()
        for j in SEND_ORDER[1:]:
            exch_u.forward(j)
        exch_u.arrived()
        exch_u.take()
        exch_d.finish()
        exch_u.finish()


def head(x_a, x_b, dy_b, gate_b, tables, weights, gain_attn, gain_moe, group, seg):
    tokens, hidden = x_a.shape
    seq_len = min(tokens, SEQ_MAX)
    seqs = tokens // seq_len
    rows_b = pl.BlockSpec((seq_len, hidden), lambda i: (jnp.minimum(i, seqs - 1), 0))
    rows_a = pl.BlockSpec((seq_len, hidden), lambda i: (jnp.maximum(i - seqs, 0), 0))
    once = pl.Buffered(1)

    def fixed(*shape):
        return pl.BlockSpec(shape, lambda i: (0,) * len(shape), pipeline_mode=once)

    def dma(*shape):
        return pltpu.SemaphoreType.DMA(shape)

    row = jax.ShapeDtypeStruct((1, tokens), jnp.int32)
    row_out = pl.BlockSpec((1, tokens), lambda i: (0, 0))
    full = jax.ShapeDtypeStruct((tokens, hidden), BF)
    slots = jax.ShapeDtypeStruct((group * seg, hidden), BF)
    exchange = [pltpu.VMEM((4 * seg, hidden), BF), pltpu.VMEM((tokens, hidden), BF), pltpu.VMEM((4, tokens, hidden), BF)]
    exchange += [dma(3), dma(3), dma(PIECES), dma(2 * PIECES), dma(2 * PIECES), dma(2 * PIECES), dma(2, 2 * PIECES)]
    scratch = [pltpu.VMEM((tokens, hidden), BF), pltpu.VMEM((1, tokens), jnp.int32), pltpu.VMEM((2 * group, 128), jnp.int32), pltpu.VMEM((4, 2 * group, 128), jnp.int32)]
    scratch += [pltpu.VMEM((seq_len, hidden), BF)] * 4 + [pltpu.VMEM((seg, hidden), BF), dma(4), dma(4), dma(2)]
    return pl.pallas_call(
        functools.partial(head_kernel, group),
        grid=(2 * seqs,),
        in_specs=[fixed(1, tokens)] * 4 + [fixed(tokens, 1), fixed(tokens, hidden), rows_a, rows_b] + [fixed(hidden, hidden)] * 4 + [fixed(1, hidden)] * 2,
        out_specs=[row_out, row_out, rows_a, pl.BlockSpec((group * seg, hidden), lambda i: (0, 0))] + [rows_b] * 5 + [pl.BlockSpec(memory_space=pl.ANY)] * 2,
        out_shape=[row, row, full, slots] + [full] * 5 + [slots, slots],
        scratch_shapes=scratch + exchange + exchange,
        compiler_params=pltpu.CompilerParams(vmem_limit_bytes=VMEM_LIMIT, dimension_semantics=('arbitrary',), collective_id=1, has_side_effects=True),
        cost_estimate=cost(10 ** 11, 60 * tokens * hidden),
        name='head',
    )(*[table.reshape(1, tokens) for table in tables], gate_b, dy_b, x_a, x_b, *weights, gain_attn[None, :], gain_moe[None, :])


def weight_specs(hidden, ff):
    up = pl.BlockSpec((hidden, ff), lambda i, n, ids: (0, 0), pipeline_mode=pl.Buffered(1))
    down = pl.BlockSpec((ff, hidden), lambda i, n, ids: (0, 0), pipeline_mode=pl.Buffered(1))
    return [up, up, down]


def pick_specs(half, hidden):
    def picked(part):
        return pl.BlockSpec((half, hidden), lambda i, n, ids: (ids[jnp.minimum(2 * i + part, jnp.maximum(n[0] - 1, 0))], 0))

    return [picked(0), picked(1)]


def join_pair(first_ref, second_ref, both):
    second = second_ref[:]
    return jnp.concatenate([first_ref[:], jnp.where(both, second, jnp.zeros_like(second))], axis=0)


def pair_loop(n_ref, ids_ref, buf, out_ref, sem, half, compute):
    step = pl.program_id(0)
    steps = pl.num_programs(0)

    def copies(at):
        slot = lax.rem(at, 2)
        return [
            pltpu.make_async_copy(
                buf.at[slot, pl.ds(part * half, half), :],
                out_ref.at[pl.ds(pl.multiple_of(ids_ref[2 * at + part] * half, half), half), :],
                sem.at[slot, part],
            )
            for part in range(2)
        ]

    def drain(at):
        for copy in copies(at):
            copy.wait()

    @pl.when(step >= 2)
    def _():
        drain(step - 2)

    dst = buf.at[lax.rem(step, 2)]

    @pl.when(2 * step < n_ref[0])
    def _():
        compute(2 * step + 1 < n_ref[0], dst)

    @pl.when(2 * step >= n_ref[0])
    def _():
        dst[:] = jnp.zeros_like(dst)

    for copy in copies(step):
        copy.start()

    @pl.when(step == steps - 1)
    def _():
        drain(step - 1)
        drain(step)


def ffn_fwd_kernel(half, chunk, n_ref, ids_ref, u0_ref, u1_ref, wg_ref, wu_ref, wd_ref, o_ref, acc, buf, sem):
    def compute(both, dst):
        u_rows = join_pair(u0_ref, u1_ref, both)
        acc[:] = jnp.zeros_like(acc)

        def body(c, carry):
            cols = pl.ds(pl.multiple_of(c * chunk, chunk), chunk)
            z_gate = mm(u_rows, wg_ref[:, cols])
            z_up = mm(u_rows, wu_ref[:, cols])
            act = (z_gate * jax.nn.sigmoid(z_gate) * z_up).astype(BF)
            acc[:] += mm(act, wd_ref[cols, :])
            return carry

        lax.fori_loop(0, wg_ref.shape[1] // chunk, body, 0, unroll=2)
        dst[:] = acc[:].astype(BF)

    pair_loop(n_ref, ids_ref, buf, o_ref, sem, half, compute)


def pair_scratch(half, hidden):
    return [pltpu.VMEM((2 * half, hidden), F32), pltpu.VMEM((2, 2 * half, hidden), BF), pltpu.SemaphoreType.DMA((2, 2))]


def ffn_forward(n_blocks, ids, u_rows, w_gate, w_up, w_down, half=128, chunk=512):
    rows, hidden = u_rows.shape
    ff = w_gate.shape[1]
    return pl.pallas_call(
        functools.partial(ffn_fwd_kernel, half, chunk),
        grid_spec=pltpu.PrefetchScalarGridSpec(
            num_scalar_prefetch=2,
            grid=(rows // (2 * half),),
            in_specs=pick_specs(half, hidden) + weight_specs(hidden, ff),
            out_specs=pl.BlockSpec(memory_space=pl.ANY),
            scratch_shapes=pair_scratch(half, hidden),
        ),
        out_shape=jax.ShapeDtypeStruct((rows, hidden), BF),
        compiler_params=params(1),
        cost_estimate=cost(3 * rows * hidden * ff, 6 * hidden * ff),
        name='ffn_fwd',
    )(n_blocks, ids, u_rows, u_rows, w_gate, w_up, w_down)


def ffn_bwd_kernel(half, chunk, n_ref, ids_ref, u0_ref, u1_ref, d0_ref, d1_ref, wg_ref, wu_ref, wd_ref, din_ref, uc_ref, dc_ref, act_ref, dzg_ref, dzu_ref, acc, buf, sem):
    def compute(both, dst):
        u_rows = join_pair(u0_ref, u1_ref, both)
        d_out = join_pair(d0_ref, d1_ref, both)
        uc_ref[:] = u_rows
        dc_ref[:] = d_out
        acc[:] = jnp.zeros_like(acc)

        def body(c, carry):
            cols = pl.ds(pl.multiple_of(c * chunk, chunk), chunk)
            z_gate = mm(u_rows, wg_ref[:, cols])
            z_up = mm(u_rows, wu_ref[:, cols])
            d_act = mm_nt(d_out, wd_ref[cols, :]).astype(BF).astype(F32)
            sig = jax.nn.sigmoid(z_gate)
            silu = z_gate * sig
            act_ref[:, cols] = (silu * z_up).astype(BF)
            d_zg = (d_act * z_up * sig * (1.0 + z_gate * (1.0 - sig))).astype(BF)
            d_zu = (d_act * silu).astype(BF)
            dzg_ref[:, cols] = d_zg
            dzu_ref[:, cols] = d_zu
            acc[:] += mm_nt(d_zg, wg_ref[:, cols]) + mm_nt(d_zu, wu_ref[:, cols])
            return carry

        lax.fori_loop(0, wg_ref.shape[1] // chunk, body, 0)
        dst[:] = acc[:].astype(BF)

    pair_loop(n_ref, ids_ref, buf, din_ref, sem, half, compute)


def step_index(n_ref, i):
    return jnp.minimum(i, jnp.maximum((n_ref[0] + 1) // 2 - 1, 0))


def ffn_backward(n_blocks, ids, u_rows, d_out, w_gate, w_up, w_down, half=128, chunk=512):
    rows, hidden = u_rows.shape
    ff = w_gate.shape[1]
    row_spec = pl.BlockSpec((2 * half, hidden), lambda i, n, ids: (step_index(n, i), 0))
    wide_spec = pl.BlockSpec((2 * half, ff), lambda i, n, ids: (step_index(n, i), 0))
    thin, wide = jax.ShapeDtypeStruct((rows, hidden), BF), jax.ShapeDtypeStruct((rows, ff), BF)
    return pl.pallas_call(
        functools.partial(ffn_bwd_kernel, half, chunk),
        grid_spec=pltpu.PrefetchScalarGridSpec(
            num_scalar_prefetch=2,
            grid=(rows // (2 * half),),
            in_specs=pick_specs(half, hidden) + pick_specs(half, hidden) + weight_specs(hidden, ff),
            out_specs=[pl.BlockSpec(memory_space=pl.ANY), row_spec, row_spec, wide_spec, wide_spec, wide_spec],
            scratch_shapes=pair_scratch(half, hidden),
        ),
        out_shape=(thin, thin, thin, wide, wide, wide),
        compiler_params=params(1),
        cost_estimate=cost(6 * rows * hidden * ff, 6 * hidden * ff + 3 * rows * ff),
        name='ffn_bwd',
    )(n_blocks, ids, u_rows, u_rows, d_out, d_out, w_gate, w_up, w_down)


def ffn_grad_kernel(half, n_ref, u_ref, d_ref, act_ref, dzg_ref, dzu_ref, dwg_ref, dwu_ref, dwd_ref):
    step = pl.program_id(1)
    block = u_ref.shape[0]
    held = (n_ref[0] + 1) // 2 * (2 * half) - step * block

    @pl.when(step == 0)
    def _():
        for grad in (dwg_ref, dwu_ref, dwd_ref):
            grad[:] = jnp.zeros_like(grad)

    def add(size):
        rows = pl.ds(0, size)
        dwg_ref[:] += mm_tn(u_ref[rows, :], dzg_ref[rows, :])
        dwu_ref[:] += mm_tn(u_ref[rows, :], dzu_ref[rows, :])
        dwd_ref[:] += mm_tn(act_ref[rows, :], d_ref[rows, :])

    @pl.when(held >= block)
    def _():
        add(block)

    @pl.when((held > 0) & (held < block))
    def _():
        add(2 * half)


def ffn_grads(n_blocks, u_rows, d_out, act, d_zg, d_zu, half, chunk=1024):
    rows, hidden = u_rows.shape
    ff = act.shape[1]
    block = 4 * half

    def last_held(n_ref, i):
        return jnp.minimum(i, jnp.maximum((n_ref[0] + 3) // 4 - 1, 0))

    row_spec = pl.BlockSpec((block, hidden), lambda j, i, n: (last_held(n, i), 0))
    wide_spec = pl.BlockSpec((block, chunk), lambda j, i, n: (last_held(n, i), j))
    up_spec = pl.BlockSpec((hidden, chunk), lambda j, i, n: (0, j))
    down_spec = pl.BlockSpec((chunk, hidden), lambda j, i, n: (j, 0))
    up = jax.ShapeDtypeStruct((hidden, ff), F32)
    return pl.pallas_call(
        functools.partial(ffn_grad_kernel, half),
        grid_spec=pltpu.PrefetchScalarGridSpec(
            num_scalar_prefetch=1,
            grid=(ff // chunk, rows // block),
            in_specs=[row_spec, row_spec, wide_spec, wide_spec, wide_spec],
            out_specs=[up_spec, up_spec, down_spec],
        ),
        out_shape=(up, up, jax.ShapeDtypeStruct((ff, hidden), F32)),
        compiler_params=params(2),
        cost_estimate=cost(3 * rows * hidden * ff, 12 * hidden * ff + 3 * rows * ff),
        name='ffn_grads',
    )(n_blocks, u_rows, d_out, act, d_zg, d_zu)


def attn_bwd_kernel(num_experts, x_ref, h_ref, dy_ref, q_ref, k_ref, v_ref, mixed_ref, back_ref, pos_ref, wq_ref, wk_ref, wv_ref, wo_ref, ga_ref, gm_ref, dx_ref, dw_ref, dq, dk, dv, dmix):
    seq_len, hidden = x_ref.shape
    d_u = unpack_rows(pos_ref[:], num_experts, back_ref).astype(BF)
    d_h = (dy_ref[:].astype(F32) + norm_back(h_ref[:].astype(F32), gm_ref[:], d_u).astype(F32)).astype(BF)
    dmix[:] = mm_nt(d_h, wo_ref[:]).astype(BF)
    causal = causal_mask(seq_len)
    for head in range(hidden // HEAD_DIM):
        cols = pl.ds(head * HEAD_DIM, HEAD_DIM)
        q_head, k_head, v_head, d_mixed = q_ref[:, cols], k_ref[:, cols], v_ref[:, cols], dmix[:, cols]
        probs = softmax_head(q_head, k_head, causal)
        d_probs = mm_nt(d_mixed, v_head)
        dv[:, cols] = mm_tn(probs.astype(BF), d_mixed).astype(BF)
        d_scores = (probs * (d_probs - jnp.sum(d_probs * probs, axis=-1, keepdims=True)) * HEAD_DIM ** -0.5).astype(BF)
        dq[:, cols] = mm(d_scores, k_head).astype(BF)
        dk[:, cols] = mm_tn(d_scores, q_head).astype(BF)
    x_f = x_ref[:].astype(F32)
    normed = norm_rows(x_f, ga_ref[:])

    @pl.when(pl.program_id(0) == 0)
    def _():
        dw_ref[:] = jnp.zeros_like(dw_ref)

    normed_t = normed.T
    dw_ref[0] += mm(normed_t, dq[:])
    dw_ref[1] += mm(normed_t, dk[:])
    dw_ref[2] += mm(normed_t, dv[:])
    dw_ref[3] += mm_tn(mixed_ref[:], d_h)
    d_normed = (mm_nt(dq[:], wq_ref[:]) + mm_nt(dk[:], wk_ref[:]) + mm_nt(dv[:], wv_ref[:])).astype(BF)
    dx_ref[:] = (d_h.astype(F32) + norm_back(x_f, ga_ref[:], d_normed).astype(F32)).astype(BF)


def attn_backward(num_experts, x_rows, h_rows, dy_rows, saved, back, pos_col, w_q, w_k, w_v, w_o, gain_attn, gain_moe):
    tokens, hidden = x_rows.shape
    seq_len = min(tokens, SEQ_MAX)
    rows = pl.BlockSpec((seq_len, hidden), lambda i: (i, 0))
    whole = pl.BlockSpec((hidden, hidden), lambda i: (0, 0))
    gain = pl.BlockSpec((1, hidden), lambda i: (0, 0))
    return pl.pallas_call(
        functools.partial(attn_bwd_kernel, num_experts),
        grid=(tokens // seq_len,),
        in_specs=[rows] * 7 + [pl.BlockSpec(back.shape, lambda i: (0, 0)), pl.BlockSpec((seq_len, 1), lambda i: (i, 0))] + [whole] * 4 + [gain] * 2,
        out_specs=[rows, pl.BlockSpec((4, hidden, hidden), lambda i: (0, 0, 0))],
        out_shape=(jax.ShapeDtypeStruct((tokens, hidden), BF), jax.ShapeDtypeStruct((4, hidden, hidden), F32)),
        scratch_shapes=[pltpu.VMEM((seq_len, hidden), BF)] * 4,
        compiler_params=params(1),
        cost_estimate=cost(26 * tokens * hidden * hidden, 40 * tokens * hidden),
        name='attn_bwd',
    )(x_rows, h_rows, dy_rows, *saved, back, pos_col, w_q, w_k, w_v, w_o, gain_attn[None, :], gain_moe[None, :])


def combine_kernel(num_experts, h_ref, back_ref, pos_ref, gate_ref, sum_ref, y_ref, *rest):
    outs, sem = rest[:-1], rest[-1]
    copies = [pltpu.make_async_copy(sum_ref, out, sem) for out in outs]

    def when_mine(act):
        for i, copy in enumerate(copies):
            @pl.when(pl.program_id(0) == i)
            def _(copy=copy):
                act(copy)

    when_mine(lambda copy: copy.start())
    picked = unpack_rows(pos_ref[:], num_experts, back_ref)
    y_ref[:] = (h_ref[:].astype(F32) + gate_ref[:].astype(F32) * picked).astype(BF)
    when_mine(lambda copy: copy.wait())


def combine(num_experts, h_rows, back, pos_col, gate_col, sums):
    tokens, hidden = h_rows.shape
    count = sums.shape[0] // hidden
    block = tokens // count
    rows = pl.BlockSpec((block, hidden), lambda i: (i, 0))
    one = pl.BlockSpec((block, 1), lambda i: (i, 0))
    return pl.pallas_call(
        functools.partial(combine_kernel, num_experts),
        grid=(count,),
        in_specs=[rows, pl.BlockSpec(back.shape, lambda i: (0, 0)), one, one, pl.BlockSpec((hidden, hidden), lambda i: (i, 0))],
        out_specs=[rows] + [pl.BlockSpec(memory_space=pl.ANY)] * count,
        out_shape=[jax.ShapeDtypeStruct((tokens, hidden), BF)] + [jax.ShapeDtypeStruct((hidden, hidden), F32)] * count,
        scratch_shapes=[pltpu.SemaphoreType.DMA],
        compiler_params=params(1),
        cost_estimate=cost(2 * tokens * tokens * hidden, 6 * tokens * hidden),
        name='combine',
    )(h_rows, back, pos_col, gate_col, sums)


def active_blocks(rows, half):
    blocks = rows.shape[0] // half
    flags = jnp.any(rows.reshape(blocks, half, rows.shape[1]) != 0, axis=(1, 2)).astype(jnp.int32)
    earlier = jnp.arange(blocks)[:, None] < jnp.arange(blocks)[None, :]
    total = jnp.sum(flags)
    rank_on = jnp.sum(jnp.where(earlier, flags[:, None], 0), axis=0)
    rank_off = total + jnp.sum(jnp.where(earlier, 1 - flags[:, None], 0), axis=0)
    rank = jnp.where(flags > 0, rank_on, rank_off)
    ids = jnp.sum(jnp.where(rank[None, :] == jnp.arange(blocks)[:, None], jnp.arange(blocks)[None, :], 0), axis=1)
    return total.astype(jnp.int32).reshape(1), ids.astype(jnp.int32)


CHUNK = 64
LAG_TOTAL = 3
LAG_FORWARD = 6


def reduce_kernel(x_ref, *rest):
    out_ref, (prt, acc, from_end, from_mid, tot, s_prt, r_prt, s_up, r_up, s_mid, r_mid, s_end, s_fwd, s_share, r_tot, r_share, s_out) = rest[0], rest[1:]
    me = lax.axis_index('ep')
    core, z = lax.rem(me, 2), me // 2
    is_mid = (z == 1) | (z == 2)
    is_end = jnp.logical_not(is_mid)
    side = z // 2
    half = acc.shape[0]
    steps = half // CHUNK
    partner = 2 * z + 1 - core
    mate = 2 * (2 * side + 1 - lax.rem(z, 2)) + core
    across = 2 * (3 - z) + core

    def send(src, dst, send_sem, recv_sem, to):
        return pltpu.make_async_remote_copy(src_ref=src, dst_ref=dst, send_sem=send_sem, recv_sem=recv_sem, device_id={'ep': to}, device_id_type=pl.DeviceIdType.MESH)

    def rows(k):
        return pl.ds(pl.multiple_of(k * CHUNK, CHUNK), CHUNK)

    def mine(k):
        return pl.ds(pl.multiple_of(core * half + k * CHUNK, CHUNK), CHUNK)

    def theirs(k):
        return pl.ds(pl.multiple_of((1 - core) * half + k * CHUNK, CHUNK), CHUNK)

    def c_prt(k):
        return send(x_ref.at[theirs(k), :], prt.at[rows(k), :], s_prt.at[k], r_prt.at[k], partner)

    def c_up(k):
        return send(acc.at[rows(k), :], from_end.at[rows(k), :], s_up.at[k], r_up.at[k], mate)

    def c_mid(k):
        return send(acc.at[rows(k), :], from_mid.at[rows(k), :], s_mid.at[k], r_mid.at[k], across)

    def c_end(k):
        return send(tot.at[mine(k), :], tot.at[mine(k), :], s_end.at[k], r_tot.at[k], mate)

    def c_fwd(k):
        return send(tot.at[mine(k), :], tot.at[mine(k), :], s_fwd.at[k], r_tot.at[k], across)

    def c_share(k):
        return send(tot.at[mine(k), :], tot.at[mine(k), :], s_share.at[k], r_share.at[k], partner)

    barrier = pltpu.get_barrier_semaphore()
    for peer in (partner, mate):
        pl.semaphore_signal(barrier, inc=1, device_id={'ep': peer}, device_id_type=pl.DeviceIdType.MESH)

    @pl.when(is_mid)
    def _():
        pl.semaphore_signal(barrier, inc=1, device_id={'ep': across}, device_id_type=pl.DeviceIdType.MESH)
        pl.semaphore_wait(barrier, 3)

    @pl.when(is_end)
    def _():
        pl.semaphore_wait(barrier, 2)

    def begin(k, carry):
        c_prt(k).start()
        return carry

    lax.fori_loop(0, steps, begin, 0)

    def chip_sum(k):
        c_prt(k).wait_recv()
        acc[rows(k), :] = x_ref[mine(k), :] + prt[rows(k), :]

    @pl.when(is_end)
    def _():
        def up(k, carry):
            chip_sum(k)
            c_up(k).start()
            return carry

        lax.fori_loop(0, steps, up, 0)

        def take(k, carry):
            c_end(k).wait_recv()
            c_share(k).start()
            return carry

        lax.fori_loop(0, steps, take, 0)

    @pl.when(is_mid)
    def _():
        def run(t, carry):
            @pl.when(t < steps)
            def _():
                chip_sum(t)
                c_up(t).wait_recv()
                acc[rows(t), :] += from_end[rows(t), :]

                @pl.when(lax.rem(t, 2) != side)
                def _():
                    c_mid(t).start()

            j = t - LAG_TOTAL

            @pl.when((j >= 0) & (j < steps) & (lax.rem(j + 2, 2) == side))
            def _():
                c_mid(j).wait_recv()
                tot[mine(j), :] = acc[rows(j), :] + from_mid[rows(j), :]
                c_fwd(j).start()
                c_end(j).start()
                c_share(j).start()

            f = t - LAG_FORWARD

            @pl.when((f >= 0) & (lax.rem(f + 6, 2) != side))
            def _():
                c_fwd(f).wait_recv()
                c_end(f).start()
                c_share(f).start()

            return carry

        lax.fori_loop(0, steps + LAG_FORWARD, run, 0)

    def finish(k, carry):
        c_share(k).wait_recv()
        c_prt(k).wait_send()
        c_share(k).wait_send()

        @pl.when(is_end)
        def _():
            c_up(k).wait_send()

        @pl.when(is_mid)
        def _():
            c_end(k).wait_send()

            @pl.when(lax.rem(k, 2) != side)
            def _():
                c_mid(k).wait_send()

            @pl.when(lax.rem(k, 2) == side)
            def _():
                c_fwd(k).wait_send()

        return carry

    lax.fori_loop(0, steps, finish, 0)
    flush = pltpu.make_async_copy(tot, out_ref, s_out)
    flush.start()
    flush.wait()


def group_sum(stacked):
    count, size, hidden = stacked.shape
    total = count * size
    half = total // 2
    steps = half // CHUNK
    dma = pltpu.SemaphoreType.DMA((steps,))
    return pl.pallas_call(
        reduce_kernel,
        in_specs=[pl.BlockSpec(memory_space=pltpu.VMEM)],
        out_specs=pl.BlockSpec(memory_space=pl.ANY),
        out_shape=jax.ShapeDtypeStruct((total, hidden), F32),
        scratch_shapes=[pltpu.VMEM((half, hidden), F32)] * 4 + [pltpu.VMEM((total, hidden), F32)] + [dma] * 11 + [pltpu.SemaphoreType.DMA],
        compiler_params=pltpu.CompilerParams(vmem_limit_bytes=VMEM_LIMIT, collective_id=0, has_side_effects=True),
        cost_estimate=cost(10 ** 11, 8 * total * hidden),
        name='group_sum',
    )(stacked.reshape(total, hidden))


def solution(mesh):
    group_size = mesh.shape['ep']
    row_spec = P(('dp', 'ep'), None)
    rep_two = P(None, None)
    rep_one = P(None)
    expert_spec = P('ep', None, None)
    grad_spec = P('dp', None)
    expert_grad_spec = P(('dp', 'ep'), None, None)

    def device_program(x_a, x_b, dy_b, w_q, w_k, w_v, w_o, gain_attn, gain_moe, w_gate, w_up, w_down, expert_a, slot_a, gate_a, expert_b, slot_b, gate_b):
        tokens, hidden = x_a.shape
        num_experts = group_size
        seg = capacity_of(tokens, 1, num_experts)
        half = seg // 3
        w_gate, w_up, w_down = w_gate[0], w_up[0], w_down[0]

        def move(rows):
            return lax.all_to_all(rows.reshape(group_size, seg, hidden), 'ep', 0, 0, tiled=True).reshape(group_size * seg, hidden)

        tables = (expert_a, slot_a, expert_b, slot_b)
        pos_a, pos_b, h_a, pack_a, h_b, *rest = head(x_a, x_b, dy_b, gate_b, tables, (w_q, w_k, w_v, w_o), gain_attn, gain_moe, group_size, seg)
        *saved_b, d_out_b, recv_b = rest
        pos_col_a, pos_col_b = pos_a.reshape(tokens, 1), pos_b.reshape(tokens, 1)
        recv_a = move(pack_a)
        n_b, ids_b = active_blocks(recv_b, half)
        d_in_b, u_c, d_c, act_b, d_zg, d_zu = ffn_backward(n_b, ids_b, recv_b, d_out_b, w_gate, w_up, w_down, half)
        d_back = move(d_in_b)
        n_a, ids_a = active_blocks(recv_a, half)
        o_a = ffn_forward(n_a, ids_a, recv_a, w_gate, w_up, w_down, half)
        back_a = move(o_a)
        d_wgate, d_wup, d_wdown = ffn_grads(n_b, u_c, d_c, act_b, d_zg, d_zu, half)

        d_x, attn_grads = attn_backward(num_experts, x_b, h_b, dy_b, saved_b, d_back, pos_col_b, w_q, w_k, w_v, w_o, gain_attn, gain_moe)
        attn_grads = group_sum(attn_grads)
        y_a, *attn_grads = combine(num_experts, h_a, back_a, pos_col_a, gate_a, attn_grads)
        return (y_a, d_x, *attn_grads, d_wgate[None], d_wup[None], d_wdown[None])

    return jax.shard_map(device_program, mesh=mesh, in_specs=(row_spec, row_spec, row_spec, rep_two, rep_two, rep_two, rep_two, rep_one, rep_one, expert_spec, expert_spec, expert_spec, row_spec, row_spec, row_spec, row_spec, row_spec, row_spec), out_specs=(row_spec, row_spec, grad_spec, grad_spec, grad_spec, grad_spec, expert_grad_spec, expert_grad_spec, expert_grad_spec), check_vma=False)
```

```python
import functools

import jax
import jax.numpy as jnp
from jax import lax
from jax.experimental import pallas as pl
from jax.experimental.pallas import tpu as pltpu
from jax.sharding import PartitionSpec as P

RMS_EPS = 1e-6
HEAD_DIM = 128
SEQ_MAX = 256
FAR = 1 << 20
BF = jnp.bfloat16
F32 = jnp.float32
VMEM_LIMIT = 60 * 1024 * 1024


def capacity_of(tokens, choices, num_experts):
    return ((3 * tokens * choices // num_experts + 7) // 8) * 8


def params(dims):
    return pltpu.CompilerParams(vmem_limit_bytes=VMEM_LIMIT, dimension_semantics=('arbitrary',) * dims)


def cost(flops, moved):
    return pl.CostEstimate(flops=flops, bytes_accessed=moved, transcendentals=0)


def one_where(condition):
    return jnp.where(condition, 1.0, 0.0).astype(BF)


def iota(shape, dim):
    return lax.broadcasted_iota(jnp.int32, shape, dim)


def mm(lhs, rhs):
    return jnp.dot(lhs, rhs, preferred_element_type=F32)


def mm_nt(lhs, rhs):
    return lax.dot_general(lhs, rhs, (((1,), (1,)), ((), ())), preferred_element_type=F32)


def mm_tn(lhs, rhs):
    return lax.dot_general(lhs, rhs, (((0,), (0,)), ((), ())), preferred_element_type=F32)


def inv_rms_of(rows_f):
    return lax.rsqrt(jnp.mean(rows_f * rows_f, axis=-1, keepdims=True) + RMS_EPS)


def norm_rows(rows_f, gain_row):
    return (rows_f * inv_rms_of(rows_f) * gain_row).astype(BF)


def norm_back(rows_f, gain_row, d_normed):
    inv = inv_rms_of(rows_f)
    scaled = d_normed.astype(F32) * gain_row
    dot_mean = jnp.mean(scaled * rows_f, axis=-1, keepdims=True)
    return (scaled * inv - rows_f * (inv * inv * inv * dot_mean)).astype(BF)


def pack_rows(pos_row, src_ref, dst_ref, chunk):
    tokens = pos_row.shape[1]

    def body(c, carry):
        base = pl.multiple_of(c * chunk, chunk)
        want = base + iota((chunk, tokens), 0)
        onehot = one_where(want == pos_row)
        dst_ref[pl.ds(base, chunk), :] = mm(onehot, src_ref[:]).astype(BF)
        return carry

    lax.fori_loop(0, dst_ref.shape[0] // chunk, body, 0)


def unpack_rows(pos_col, num_experts, back_ref):
    seg = back_ref.shape[0] // num_experts
    total = jnp.zeros((pos_col.shape[0], back_ref.shape[1]), F32)
    for e in range(num_experts):
        want = e * seg + iota((pos_col.shape[0], seg), 1)
        total += mm(one_where(want == pos_col), back_ref[pl.ds(e * seg, seg), :])
    return total


def route_one(e_ref, s_ref, pos_ref, num_experts, seg):
    tokens = e_ref.shape[1]
    expert = e_ref[:]
    kept = s_ref[:] >= 0
    sub_expert = iota((num_experts, tokens), 0)
    onehot_f = jnp.where((sub_expert == expert) & kept, 1.0, 0.0)
    onehot = onehot_f.astype(BF)
    before = iota((tokens, tokens), 0) < iota((tokens, tokens), 1)
    rank = mm(onehot, one_where(before))
    pos = expert * seg + jnp.sum(onehot_f * rank, axis=0, keepdims=True).astype(jnp.int32)
    pos_ref[:] = jnp.where(kept, pos, FAR)
    return expert, kept, onehot_f, rank


def softmax_head(q_head, k_head, causal):
    scores = jnp.where(causal, mm_nt(q_head, k_head) * HEAD_DIM ** -0.5, -1e30)
    expd = jnp.exp(scores - jnp.max(scores, axis=-1, keepdims=True))
    return expd * (1.0 / jnp.sum(expd, axis=-1, keepdims=True))


def causal_mask(seq_len):
    return iota((seq_len, seq_len), 0) >= iota((seq_len, seq_len), 1)


def attn_rows(x_ref, w_refs, ga_ref, gm_ref, h_ref, q_ref, k_ref, v_ref, mixed_ref, u_all, seq):
    wq_ref, wk_ref, wv_ref, wo_ref = w_refs
    seq_len, hidden = x_ref.shape
    x_f = x_ref[:].astype(F32)
    normed = norm_rows(x_f, ga_ref[:])
    q_ref[:] = mm(normed, wq_ref[:]).astype(BF)
    k_ref[:] = mm(normed, wk_ref[:]).astype(BF)
    v_ref[:] = mm(normed, wv_ref[:]).astype(BF)
    causal = causal_mask(seq_len)
    for head in range(hidden // HEAD_DIM):
        cols = pl.ds(head * HEAD_DIM, HEAD_DIM)
        probs = softmax_head(q_ref[:, cols], k_ref[:, cols], causal).astype(BF)
        mixed_ref[:, cols] = mm(probs, v_ref[:, cols]).astype(BF)
    h_rows = (x_f + mm(mixed_ref[:], wo_ref[:])).astype(BF)
    h_ref[:] = h_rows
    u_all[pl.ds(pl.multiple_of(seq * seq_len, seq_len), seq_len), :] = norm_rows(h_rows.astype(F32), gm_ref[:])


PIECES = 4
SEND_ORDER = (1, 2, 3, 0)


def head_kernel(group, ea_ref, sa_ref, eb_ref, sb_ref, gate_ref, dy_ref, xa_ref, xb_ref, wq_ref, wk_ref, wv_ref, wo_ref, ga_ref, gm_ref,
                pos_a_ref, pos_b_ref, ha_ref, pack_a_ref, hb_ref, q_ref, k_ref, v_ref, mixed_ref, recv_d_ref, recv_u_ref,
                rows_all, pos_cross, meta, meta_in, qa, ka, va, ma, slot_rows, s_meta, r_meta, own, *buffers):
    step = pl.program_id(0)
    seqs = pl.num_programs(0) // 2
    me = lax.axis_index('ep')
    core, chip = lax.rem(me, 2), me // 2
    side = chip // 2
    local = lax.rem(me, 4)
    is_mid = (chip == 1) | (chip == 2)
    is_end = jnp.logical_not(is_mid)
    partner = 2 * chip + 1 - core
    relay = 2 * (2 - side) + core
    end_dev = 2 * (3 * side) + core
    tokens = rows_all.shape[0]
    seg = slot_rows.shape[1]
    piece = tokens // PIECES
    w_refs = (wq_ref, wk_ref, wv_ref, wo_ref)
    tensors = (buffers[:10] + (recv_d_ref, 0), buffers[10:] + (recv_u_ref, 1))

    def remote(src, dst, send_sem, recv_sem, to):
        return pltpu.make_async_remote_copy(src_ref=src, dst_ref=dst, send_sem=send_sem, recv_sem=recv_sem, device_id={'ep': to}, device_id_type=pl.DeviceIdType.MESH)

    def part(index, size):
        return pl.ds(pl.multiple_of(index * size, size), size)

    class Exchange:
        def __init__(self, refs):
            (self.near, self.cross, self.win, self.s_near, self.r_near, self.s_cross, self.r_cross, self.s_end, self.r_end, self.pair, self.recv, self.which) = refs
            self.s_pair, self.r_pair = self.pair.at[0], self.pair.at[1]

        def near_copy(self, shift):
            to = lax.rem(local + shift, 4)
            return remote(self.near.at[part(to, seg), :], self.recv.at[part(me, seg), :], self.s_near.at[shift - 1], self.r_near.at[shift - 1], 4 * side + to)

        def self_copy(self):
            return pltpu.make_async_copy(self.near.at[part(local, seg), :], self.recv.at[part(me, seg), :], own.at[self.which, 4])

        def flush(self, source):
            return pltpu.make_async_copy(slot_rows.at[source], self.recv.at[part(4 * (1 - side) + source, seg), :], own.at[self.which, source])

        def cross_copy(self, a, j):
            at = part(j, piece)
            return remote(self.cross.at[at, :], self.win.at[2 * a + core, at, :], self.s_cross.at[j], self.r_cross.at[a * PIECES + j], relay)

        def end_copy(self, a, j):
            at = self.win.at[2 * a + core, pl.ds(j * piece, piece), :]
            return remote(at, at, self.s_end.at[a * PIECES + j], self.r_end.at[a * PIECES + j], end_dev)

        def pair_copy(self, a, j, whose):
            at = self.win.at[2 * a + whose, pl.ds(j * piece, piece), :]
            return remote(at, at, self.s_pair.at[a * PIECES + j], self.r_pair.at[a * PIECES + j], partner)

        def pack_and_send(self, pos_row, cross_row):
            def pack_for(row, base, size, dst):
                want = base + iota((size, tokens), 0)
                dst[:] = mm(one_where(want == row), rows_all[:]).astype(BF)

            def cross_body(i, carry):
                j = lax.rem(i + SEND_ORDER[0], PIECES)
                pack_for(cross_row, j * piece, piece, self.cross.at[part(j, piece), :])
                self.cross_copy(chip - 2 * side, j).start()
                return carry

            lax.fori_loop(0, PIECES, cross_body, 0)

            def body(shift, carry):
                to = lax.rem(local + shift, 4)
                pack_for(pos_row, (4 * side + to) * seg, seg, self.near.at[part(to, seg), :])
                self.near_copy(shift).start()
                return carry

            lax.fori_loop(1, 4, body, 0)
            pack_for(pos_row, me * seg, seg, self.near.at[part(local, seg), :])
            self.self_copy().start()

        def forward(self, j):
            @pl.when(is_mid)
            def _():
                for a in range(2):
                    self.cross_copy(a, j).wait_recv()
                    if j > 0:
                        self.end_copy(a, j).start()
                    if j < PIECES - 1:
                        self.pair_copy(a, j, core).start()

            if j > 0:
                @pl.when(is_end)
                def _():
                    for a in range(2):
                        self.end_copy(a, j).wait_recv()
                        self.pair_copy(a, j, core).start()

        def arrived(self):
            for role, pieces in ((is_mid, range(PIECES - 1)), (is_end, range(1, PIECES))):
                @pl.when(role)
                def _(pieces=pieces):
                    for a in range(2):
                        for j in pieces:
                            self.pair_copy(a, j, 1 - core).wait_recv()

        def take(self):
            base = jnp.where(is_mid, 0, piece)

            def body(source, carry):
                first = meta_in[source, pl.ds(me, 1), :][:, :1]
                count = meta_in[source, pl.ds(group + me, 1), :][:, :1]
                window = self.win[source, pl.ds(pl.multiple_of(base, piece), tokens - piece), :]
                slot = iota((seg, tokens - piece), 0)
                lane = base + iota((seg, tokens - piece), 1)
                pick = one_where((lane == first + slot) & (slot < count))
                slot_rows[source] = mm(pick, window).astype(BF)
                self.flush(source).start()
                return carry

            lax.fori_loop(0, 4, body, 0)

        def flushed(self):
            for source in range(4):
                self.flush(source).wait()

        def finish(self):
            for shift in range(1, 4):
                self.near_copy(shift).wait_recv()
                self.near_copy(shift).wait_send()
            for j in range(PIECES):
                self.cross_copy(chip - 2 * side, j).wait_send()
            for role, pieces in ((is_mid, range(PIECES - 1)), (is_end, range(1, PIECES))):
                @pl.when(role)
                def _(pieces=pieces):
                    for a in range(2):
                        for j in pieces:
                            self.pair_copy(a, j, core).wait_send()

            @pl.when(is_mid)
            def _():
                for a in range(2):
                    for j in range(1, PIECES):
                        self.end_copy(a, j).wait_send()

    exch_d, exch_u = Exchange(tensors[0]), Exchange(tensors[1])

    def meta_copy(shift):
        to = 4 * (1 - side) + lax.rem(local + shift, 4)
        return remote(meta, meta_in.at[local], s_meta.at[shift], r_meta.at[shift], to)

    @pl.when(step == 0)
    def _():
        barrier = pltpu.get_barrier_semaphore()

        def greet(shift, carry):
            pl.semaphore_signal(barrier, inc=1, device_id={'ep': lax.rem(me + shift, group)}, device_id_type=pl.DeviceIdType.MESH)
            return carry

        lax.fori_loop(1, group, greet, 0)
        expert, kept, onehot_f, rank = route_one(eb_ref, sb_ref, pos_b_ref, group, seg)
        row_e = iota((group, group), 0)
        col_e = iota((group, group), 1)
        row_mid = (row_e >= 2) & (row_e < 6)
        same_chip = (row_e // 2) == (col_e // 2)
        reach = jnp.where(same_chip & ((row_mid & (col_e < row_e)) | (jnp.logical_not(row_mid) & (col_e >= row_e))), 1.0, 0.0).astype(BF)
        reached = jnp.sum(mm(reach, onehot_f.astype(BF)), axis=1, keepdims=True)
        one_e = iota((group, 1), 0)
        start = jnp.where((one_e >= 2) & (one_e < 6), reached, tokens - reached)
        count = jnp.sum(onehot_f, axis=1, keepdims=True)
        meta[pl.ds(0, group), :] = jnp.broadcast_to(start.astype(jnp.int32), (group, 128))
        meta[pl.ds(group, group), :] = jnp.broadcast_to(count.astype(jnp.int32), (group, 128))
        at = jnp.sum(onehot_f * (start + rank), axis=0, keepdims=True).astype(jnp.int32)
        pos_cross[:] = jnp.where(kept & ((expert // 4) != side), at, FAR)
        rows_all[:] = (dy_ref[:].astype(F32) * gate_ref[:].astype(F32)).astype(BF)
        pl.semaphore_wait(barrier, group - 1)
        for shift in range(4):
            meta_copy(shift).start()
        exch_d.pack_and_send(pos_b_ref[:], pos_cross[:])

    @pl.when(step < seqs)
    def _():
        attn_rows(xb_ref, w_refs, ga_ref, gm_ref, hb_ref, q_ref, k_ref, v_ref, mixed_ref, rows_all, step)

    @pl.when(step == seqs - 1)
    def _():
        exch_u.pack_and_send(pos_b_ref[:], pos_cross[:])

    for late, j in enumerate(SEND_ORDER):
        @pl.when(step == seqs - 2 + late)
        def _(j=j):
            exch_d.forward(j)

    @pl.when(step >= seqs)
    def _():
        attn_rows(xa_ref, w_refs, ga_ref, gm_ref, ha_ref, qa, ka, va, ma, rows_all, step - seqs)

    @pl.when(step == 2 * seqs - 1)
    def _():
        route_one(ea_ref, sa_ref, pos_a_ref, group, seg)
        pack_rows(pos_a_ref[:], rows_all, pack_a_ref, seg)
        exch_u.forward(SEND_ORDER[0])
        for shift in range(4):
            meta_copy(shift).wait_recv()
            meta_copy(shift).wait_send()
        exch_d.self_copy().wait()
        exch_u.self_copy().wait()
        exch_d.arrived()
        exch_d.take()
        for j in SEND_ORDER[1:]:
            exch_u.forward(j)
        exch_u.arrived()
        exch_d.flushed()
        exch_u.take()
        exch_d.finish()
        exch_u.finish()
        exch_u.flushed()


def head(x_a, x_b, dy_b, gate_b, tables, weights, gain_attn, gain_moe, group, seg):
    tokens, hidden = x_a.shape
    seq_len = min(tokens, SEQ_MAX)
    seqs = tokens // seq_len
    rows_b = pl.BlockSpec((seq_len, hidden), lambda i: (jnp.minimum(i, seqs - 1), 0))
    rows_a = pl.BlockSpec((seq_len, hidden), lambda i: (jnp.maximum(i - seqs, 0), 0))
    once = pl.Buffered(1)

    def fixed(*shape):
        return pl.BlockSpec(shape, lambda i: (0,) * len(shape), pipeline_mode=once)

    def dma(*shape):
        return pltpu.SemaphoreType.DMA(shape)

    row = jax.ShapeDtypeStruct((1, tokens), jnp.int32)
    row_out = pl.BlockSpec((1, tokens), lambda i: (0, 0))
    full = jax.ShapeDtypeStruct((tokens, hidden), BF)
    slots = jax.ShapeDtypeStruct((group * seg, hidden), BF)
    exchange = [pltpu.VMEM((4 * seg, hidden), BF), pltpu.VMEM((tokens, hidden), BF), pltpu.VMEM((4, tokens, hidden), BF)]
    exchange += [dma(3), dma(3), dma(PIECES), dma(2 * PIECES), dma(2 * PIECES), dma(2 * PIECES), dma(2, 2 * PIECES)]
    scratch = [pltpu.VMEM((tokens, hidden), BF), pltpu.VMEM((1, tokens), jnp.int32), pltpu.VMEM((2 * group, 128), jnp.int32), pltpu.VMEM((4, 2 * group, 128), jnp.int32)]
    scratch += [pltpu.VMEM((seq_len, hidden), BF)] * 4 + [pltpu.VMEM((4, seg, hidden), BF), dma(4), dma(4), dma(2, 5)]
    return pl.pallas_call(
        functools.partial(head_kernel, group),
        grid=(2 * seqs,),
        in_specs=[fixed(1, tokens)] * 4 + [fixed(tokens, 1), fixed(tokens, hidden), rows_a, rows_b] + [fixed(hidden, hidden)] * 4 + [fixed(1, hidden)] * 2,
        out_specs=[row_out, row_out, rows_a, pl.BlockSpec((group * seg, hidden), lambda i: (0, 0))] + [rows_b] * 5 + [pl.BlockSpec(memory_space=pl.ANY)] * 2,
        out_shape=[row, row, full, slots] + [full] * 5 + [slots, slots],
        scratch_shapes=scratch + exchange + exchange,
        compiler_params=pltpu.CompilerParams(vmem_limit_bytes=VMEM_LIMIT, dimension_semantics=('arbitrary',), collective_id=1, has_side_effects=True),
        cost_estimate=cost(10 ** 11, 60 * tokens * hidden),
        name='head',
    )(*[table.reshape(1, tokens) for table in tables], gate_b, dy_b, x_a, x_b, *weights, gain_attn[None, :], gain_moe[None, :])


def weight_specs(hidden, ff):
    up = pl.BlockSpec((hidden, ff), lambda i, n, ids: (0, 0), pipeline_mode=pl.Buffered(1))
    down = pl.BlockSpec((ff, hidden), lambda i, n, ids: (0, 0), pipeline_mode=pl.Buffered(1))
    return [up, up, down]


def pick_specs(half, hidden):
    def picked(part):
        return pl.BlockSpec((half, hidden), lambda i, n, ids: (ids[jnp.minimum(2 * i + part, jnp.maximum(n[0] - 1, 0))], 0))

    return [picked(0), picked(1)]


def join_pair(first_ref, second_ref, both):
    second = second_ref[:]
    return jnp.concatenate([first_ref[:], jnp.where(both, second, jnp.zeros_like(second))], axis=0)


def pair_loop(n_ref, ids_ref, buf, out_ref, sem, half, compute):
    step = pl.program_id(0)
    steps = pl.num_programs(0)

    def copies(at):
        slot = lax.rem(at, 2)
        return [
            pltpu.make_async_copy(
                buf.at[slot, pl.ds(part * half, half), :],
                out_ref.at[pl.ds(pl.multiple_of(ids_ref[2 * at + part] * half, half), half), :],
                sem.at[slot, part],
            )
            for part in range(2)
        ]

    def drain(at):
        for copy in copies(at):
            copy.wait()

    @pl.when(step >= 2)
    def _():
        drain(step - 2)

    dst = buf.at[lax.rem(step, 2)]

    @pl.when(2 * step < n_ref[0])
    def _():
        compute(2 * step + 1 < n_ref[0], dst)

    @pl.when(2 * step >= n_ref[0])
    def _():
        dst[:] = jnp.zeros_like(dst)

    for copy in copies(step):
        copy.start()

    @pl.when(step == steps - 1)
    def _():
        drain(step - 1)
        drain(step)


def ffn_fwd_kernel(half, chunk, n_ref, ids_ref, u0_ref, u1_ref, wg_ref, wu_ref, wd_ref, o_ref, acc, buf, sem):
    def compute(both, dst):
        u_rows = join_pair(u0_ref, u1_ref, both)
        acc[:] = jnp.zeros_like(acc)

        def body(c, carry):
            cols = pl.ds(pl.multiple_of(c * chunk, chunk), chunk)
            z_gate = mm(u_rows, wg_ref[:, cols])
            z_up = mm(u_rows, wu_ref[:, cols])
            act = (z_gate * jax.nn.sigmoid(z_gate) * z_up).astype(BF)
            acc[:] += mm(act, wd_ref[cols, :])
            return carry

        lax.fori_loop(0, wg_ref.shape[1] // chunk, body, 0, unroll=2)
        dst[:] = acc[:].astype(BF)

    pair_loop(n_ref, ids_ref, buf, o_ref, sem, half, compute)


def pair_scratch(half, hidden):
    return [pltpu.VMEM((2 * half, hidden), F32), pltpu.VMEM((2, 2 * half, hidden), BF), pltpu.SemaphoreType.DMA((2, 2))]


def ffn_forward(n_blocks, ids, u_rows, w_gate, w_up, w_down, half=128, chunk=512):
    rows, hidden = u_rows.shape
    ff = w_gate.shape[1]
    return pl.pallas_call(
        functools.partial(ffn_fwd_kernel, half, chunk),
        grid_spec=pltpu.PrefetchScalarGridSpec(
            num_scalar_prefetch=2,
            grid=(rows // (2 * half),),
            in_specs=pick_specs(half, hidden) + weight_specs(hidden, ff),
            out_specs=pl.BlockSpec(memory_space=pl.ANY),
            scratch_shapes=pair_scratch(half, hidden),
        ),
        out_shape=jax.ShapeDtypeStruct((rows, hidden), BF),
        compiler_params=params(1),
        cost_estimate=cost(3 * rows * hidden * ff, 6 * hidden * ff),
        name='ffn_fwd',
    )(n_blocks, ids, u_rows, u_rows, w_gate, w_up, w_down)


def ffn_bwd_kernel(half, chunk, n_ref, ids_ref, u0_ref, u1_ref, d0_ref, d1_ref, wg_ref, wu_ref, wd_ref, din_ref, uc_ref, dc_ref, act_ref, dzg_ref, dzu_ref, acc, buf, sem):
    def compute(both, dst):
        u_rows = join_pair(u0_ref, u1_ref, both)
        d_out = join_pair(d0_ref, d1_ref, both)
        uc_ref[:] = u_rows
        dc_ref[:] = d_out
        acc[:] = jnp.zeros_like(acc)

        def body(c, carry):
            cols = pl.ds(pl.multiple_of(c * chunk, chunk), chunk)
            z_gate = mm(u_rows, wg_ref[:, cols])
            z_up = mm(u_rows, wu_ref[:, cols])
            d_act = mm_nt(d_out, wd_ref[cols, :]).astype(BF).astype(F32)
            sig = jax.nn.sigmoid(z_gate)
            silu = z_gate * sig
            act_ref[:, cols] = (silu * z_up).astype(BF)
            d_zg = (d_act * z_up * sig * (1.0 + z_gate * (1.0 - sig))).astype(BF)
            d_zu = (d_act * silu).astype(BF)
            dzg_ref[:, cols] = d_zg
            dzu_ref[:, cols] = d_zu
            acc[:] += mm_nt(d_zg, wg_ref[:, cols]) + mm_nt(d_zu, wu_ref[:, cols])
            return carry

        lax.fori_loop(0, wg_ref.shape[1] // chunk, body, 0)
        dst[:] = acc[:].astype(BF)

    pair_loop(n_ref, ids_ref, buf, din_ref, sem, half, compute)


def step_index(n_ref, i):
    return jnp.minimum(i, jnp.maximum((n_ref[0] + 1) // 2 - 1, 0))


def ffn_backward(n_blocks, ids, u_rows, d_out, w_gate, w_up, w_down, half=128, chunk=512):
    rows, hidden = u_rows.shape
    ff = w_gate.shape[1]
    row_spec = pl.BlockSpec((2 * half, hidden), lambda i, n, ids: (step_index(n, i), 0))
    wide_spec = pl.BlockSpec((2 * half, ff), lambda i, n, ids: (step_index(n, i), 0))
    thin, wide = jax.ShapeDtypeStruct((rows, hidden), BF), jax.ShapeDtypeStruct((rows, ff), BF)
    return pl.pallas_call(
        functools.partial(ffn_bwd_kernel, half, chunk),
        grid_spec=pltpu.PrefetchScalarGridSpec(
            num_scalar_prefetch=2,
            grid=(rows // (2 * half),),
            in_specs=pick_specs(half, hidden) + pick_specs(half, hidden) + weight_specs(hidden, ff),
            out_specs=[pl.BlockSpec(memory_space=pl.ANY), row_spec, row_spec, wide_spec, wide_spec, wide_spec],
            scratch_shapes=pair_scratch(half, hidden),
        ),
        out_shape=(thin, thin, thin, wide, wide, wide),
        compiler_params=params(1),
        cost_estimate=cost(6 * rows * hidden * ff, 6 * hidden * ff + 3 * rows * ff),
        name='ffn_bwd',
    )(n_blocks, ids, u_rows, u_rows, d_out, d_out, w_gate, w_up, w_down)


def ffn_grad_kernel(half, n_ref, u_ref, d_ref, act_ref, dzg_ref, dzu_ref, dwg_ref, dwu_ref, dwd_ref):
    step = pl.program_id(1)
    block = u_ref.shape[0]
    held = (n_ref[0] + 1) // 2 * (2 * half) - step * block

    @pl.when(step == 0)
    def _():
        for grad in (dwg_ref, dwu_ref, dwd_ref):
            grad[:] = jnp.zeros_like(grad)

    def add(size):
        rows = pl.ds(0, size)
        dwg_ref[:] += mm_tn(u_ref[rows, :], dzg_ref[rows, :])
        dwu_ref[:] += mm_tn(u_ref[rows, :], dzu_ref[rows, :])
        dwd_ref[:] += mm_tn(act_ref[rows, :], d_ref[rows, :])

    @pl.when(held >= block)
    def _():
        add(block)

    @pl.when((held > 0) & (held < block))
    def _():
        add(2 * half)


def ffn_grads(n_blocks, u_rows, d_out, act, d_zg, d_zu, half, chunk=1024):
    rows, hidden = u_rows.shape
    ff = act.shape[1]
    block = 4 * half

    def last_held(n_ref, i):
        return jnp.minimum(i, jnp.maximum((n_ref[0] + 3) // 4 - 1, 0))

    row_spec = pl.BlockSpec((block, hidden), lambda j, i, n: (last_held(n, i), 0))
    wide_spec = pl.BlockSpec((block, chunk), lambda j, i, n: (last_held(n, i), j))
    up_spec = pl.BlockSpec((hidden, chunk), lambda j, i, n: (0, j))
    down_spec = pl.BlockSpec((chunk, hidden), lambda j, i, n: (j, 0))
    up = jax.ShapeDtypeStruct((hidden, ff), F32)
    return pl.pallas_call(
        functools.partial(ffn_grad_kernel, half),
        grid_spec=pltpu.PrefetchScalarGridSpec(
            num_scalar_prefetch=1,
            grid=(ff // chunk, rows // block),
            in_specs=[row_spec, row_spec, wide_spec, wide_spec, wide_spec],
            out_specs=[up_spec, up_spec, down_spec],
        ),
        out_shape=(up, up, jax.ShapeDtypeStruct((ff, hidden), F32)),
        compiler_params=params(2),
        cost_estimate=cost(3 * rows * hidden * ff, 12 * hidden * ff + 3 * rows * ff),
        name='ffn_grads',
    )(n_blocks, u_rows, d_out, act, d_zg, d_zu)


def attn_bwd_kernel(num_experts, x_ref, h_ref, dy_ref, q_ref, k_ref, v_ref, mixed_ref, back_ref, pos_ref, wq_ref, wk_ref, wv_ref, wo_ref, ga_ref, gm_ref, dx_ref, dw_ref, dq, dk, dv, dmix):
    seq_len, hidden = x_ref.shape
    d_u = unpack_rows(pos_ref[:], num_experts, back_ref).astype(BF)
    d_h = (dy_ref[:].astype(F32) + norm_back(h_ref[:].astype(F32), gm_ref[:], d_u).astype(F32)).astype(BF)
    dmix[:] = mm_nt(d_h, wo_ref[:]).astype(BF)
    causal = causal_mask(seq_len)
    for head in range(hidden // HEAD_DIM):
        cols = pl.ds(head * HEAD_DIM, HEAD_DIM)
        q_head, k_head, v_head, d_mixed = q_ref[:, cols], k_ref[:, cols], v_ref[:, cols], dmix[:, cols]
        probs = softmax_head(q_head, k_head, causal)
        d_probs = mm_nt(d_mixed, v_head)
        dv[:, cols] = mm_tn(probs.astype(BF), d_mixed).astype(BF)
        d_scores = (probs * (d_probs - jnp.sum(d_probs * probs, axis=-1, keepdims=True)) * HEAD_DIM ** -0.5).astype(BF)
        dq[:, cols] = mm(d_scores, k_head).astype(BF)
        dk[:, cols] = mm_tn(d_scores, q_head).astype(BF)
    x_f = x_ref[:].astype(F32)
    normed = norm_rows(x_f, ga_ref[:])

    @pl.when(pl.program_id(0) == 0)
    def _():
        dw_ref[:] = jnp.zeros_like(dw_ref)

    normed_t = normed.T
    dw_ref[0] += mm(normed_t, dq[:])
    dw_ref[1] += mm(normed_t, dk[:])
    dw_ref[2] += mm(normed_t, dv[:])
    dw_ref[3] += mm_tn(mixed_ref[:], d_h)
    d_normed = (mm_nt(dq[:], wq_ref[:]) + mm_nt(dk[:], wk_ref[:]) + mm_nt(dv[:], wv_ref[:])).astype(BF)
    dx_ref[:] = (d_h.astype(F32) + norm_back(x_f, ga_ref[:], d_normed).astype(F32)).astype(BF)


def attn_backward(num_experts, x_rows, h_rows, dy_rows, saved, back, pos_col, w_q, w_k, w_v, w_o, gain_attn, gain_moe):
    tokens, hidden = x_rows.shape
    seq_len = min(tokens, SEQ_MAX)
    rows = pl.BlockSpec((seq_len, hidden), lambda i: (i, 0))
    whole = pl.BlockSpec((hidden, hidden), lambda i: (0, 0))
    gain = pl.BlockSpec((1, hidden), lambda i: (0, 0))
    return pl.pallas_call(
        functools.partial(attn_bwd_kernel, num_experts),
        grid=(tokens // seq_len,),
        in_specs=[rows] * 7 + [pl.BlockSpec(back.shape, lambda i: (0, 0)), pl.BlockSpec((seq_len, 1), lambda i: (i, 0))] + [whole] * 4 + [gain] * 2,
        out_specs=[rows, pl.BlockSpec((4, hidden, hidden), lambda i: (0, 0, 0))],
        out_shape=(jax.ShapeDtypeStruct((tokens, hidden), BF), jax.ShapeDtypeStruct((4, hidden, hidden), F32)),
        scratch_shapes=[pltpu.VMEM((seq_len, hidden), BF)] * 4,
        compiler_params=params(1),
        cost_estimate=cost(26 * tokens * hidden * hidden, 40 * tokens * hidden),
        name='attn_bwd',
    )(x_rows, h_rows, dy_rows, *saved, back, pos_col, w_q, w_k, w_v, w_o, gain_attn[None, :], gain_moe[None, :])


def combine_kernel(num_experts, h_ref, back_ref, pos_ref, gate_ref, sum_ref, y_ref, *rest):
    outs, sem = rest[:-1], rest[-1]
    copies = [pltpu.make_async_copy(sum_ref, out, sem) for out in outs]

    def when_mine(act):
        for i, copy in enumerate(copies):
            @pl.when(pl.program_id(0) == i)
            def _(copy=copy):
                act(copy)

    when_mine(lambda copy: copy.start())
    picked = unpack_rows(pos_ref[:], num_experts, back_ref)
    y_ref[:] = (h_ref[:].astype(F32) + gate_ref[:].astype(F32) * picked).astype(BF)
    when_mine(lambda copy: copy.wait())


def combine(num_experts, h_rows, back, pos_col, gate_col, sums):
    tokens, hidden = h_rows.shape
    count = sums.shape[0] // hidden
    block = tokens // count
    rows = pl.BlockSpec((block, hidden), lambda i: (i, 0))
    one = pl.BlockSpec((block, 1), lambda i: (i, 0))
    return pl.pallas_call(
        functools.partial(combine_kernel, num_experts),
        grid=(count,),
        in_specs=[rows, pl.BlockSpec(back.shape, lambda i: (0, 0)), one, one, pl.BlockSpec((hidden, hidden), lambda i: (i, 0))],
        out_specs=[rows] + [pl.BlockSpec(memory_space=pl.ANY)] * count,
        out_shape=[jax.ShapeDtypeStruct((tokens, hidden), BF)] + [jax.ShapeDtypeStruct((hidden, hidden), F32)] * count,
        scratch_shapes=[pltpu.SemaphoreType.DMA],
        compiler_params=params(1),
        cost_estimate=cost(2 * tokens * tokens * hidden, 6 * tokens * hidden),
        name='combine',
    )(h_rows, back, pos_col, gate_col, sums)


def active_blocks(rows, half):
    blocks = rows.shape[0] // half
    flags = jnp.any(rows.reshape(blocks, half, rows.shape[1]) != 0, axis=(1, 2)).astype(jnp.int32)
    earlier = jnp.arange(blocks)[:, None] < jnp.arange(blocks)[None, :]
    total = jnp.sum(flags)
    rank_on = jnp.sum(jnp.where(earlier, flags[:, None], 0), axis=0)
    rank_off = total + jnp.sum(jnp.where(earlier, 1 - flags[:, None], 0), axis=0)
    rank = jnp.where(flags > 0, rank_on, rank_off)
    ids = jnp.sum(jnp.where(rank[None, :] == jnp.arange(blocks)[:, None], jnp.arange(blocks)[None, :], 0), axis=1)
    return total.astype(jnp.int32).reshape(1), ids.astype(jnp.int32)


CHUNK = 64
LAG_TOTAL = 3
LAG_FORWARD = 6


def reduce_kernel(x_ref, *rest):
    out_ref, (prt, acc, from_end, from_mid, tot, s_prt, r_prt, s_up, r_up, s_mid, r_mid, s_end, s_fwd, s_share, r_tot, r_share, s_out) = rest[0], rest[1:]
    me = lax.axis_index('ep')
    core, z = lax.rem(me, 2), me // 2
    is_mid = (z == 1) | (z == 2)
    is_end = jnp.logical_not(is_mid)
    side = z // 2
    half = acc.shape[0]
    steps = half // CHUNK
    partner = 2 * z + 1 - core
    mate = 2 * (2 * side + 1 - lax.rem(z, 2)) + core
    across = 2 * (3 - z) + core

    def send(src, dst, send_sem, recv_sem, to):
        return pltpu.make_async_remote_copy(src_ref=src, dst_ref=dst, send_sem=send_sem, recv_sem=recv_sem, device_id={'ep': to}, device_id_type=pl.DeviceIdType.MESH)

    def rows(k):
        return pl.ds(pl.multiple_of(k * CHUNK, CHUNK), CHUNK)

    def mine(k):
        return pl.ds(pl.multiple_of(core * half + k * CHUNK, CHUNK), CHUNK)

    def theirs(k):
        return pl.ds(pl.multiple_of((1 - core) * half + k * CHUNK, CHUNK), CHUNK)

    def c_prt(k):
        return send(x_ref.at[theirs(k), :], prt.at[rows(k), :], s_prt.at[k], r_prt.at[k], partner)

    def c_up(k):
        return send(acc.at[rows(k), :], from_end.at[rows(k), :], s_up.at[k], r_up.at[k], mate)

    def c_mid(k):
        return send(acc.at[rows(k), :], from_mid.at[rows(k), :], s_mid.at[k], r_mid.at[k], across)

    def c_end(k):
        return send(tot.at[mine(k), :], tot.at[mine(k), :], s_end.at[k], r_tot.at[k], mate)

    def c_fwd(k):
        return send(tot.at[mine(k), :], tot.at[mine(k), :], s_fwd.at[k], r_tot.at[k], across)

    def c_share(k):
        return send(tot.at[mine(k), :], tot.at[mine(k), :], s_share.at[k], r_share.at[k], partner)

    barrier = pltpu.get_barrier_semaphore()
    for peer in (partner, mate):
        pl.semaphore_signal(barrier, inc=1, device_id={'ep': peer}, device_id_type=pl.DeviceIdType.MESH)

    @pl.when(is_mid)
    def _():
        pl.semaphore_signal(barrier, inc=1, device_id={'ep': across}, device_id_type=pl.DeviceIdType.MESH)
        pl.semaphore_wait(barrier, 3)

    @pl.when(is_end)
    def _():
        pl.semaphore_wait(barrier, 2)

    def begin(k, carry):
        c_prt(k).start()
        return carry

    lax.fori_loop(0, steps, begin, 0)

    def chip_sum(k):
        c_prt(k).wait_recv()
        acc[rows(k), :] = x_ref[mine(k), :] + prt[rows(k), :]

    @pl.when(is_end)
    def _():
        def up(k, carry):
            chip_sum(k)
            c_up(k).start()
            return carry

        lax.fori_loop(0, steps, up, 0)

        def take(k, carry):
            c_end(k).wait_recv()
            c_share(k).start()
            return carry

        lax.fori_loop(0, steps, take, 0)

    @pl.when(is_mid)
    def _():
        def run(t, carry):
            @pl.when(t < steps)
            def _():
                chip_sum(t)
                c_up(t).wait_recv()
                acc[rows(t), :] += from_end[rows(t), :]

                @pl.when(lax.rem(t, 2) != side)
                def _():
                    c_mid(t).start()

            j = t - LAG_TOTAL

            @pl.when((j >= 0) & (j < steps) & (lax.rem(j + 2, 2) == side))
            def _():
                c_mid(j).wait_recv()
                tot[mine(j), :] = acc[rows(j), :] + from_mid[rows(j), :]
                c_fwd(j).start()
                c_end(j).start()
                c_share(j).start()

            f = t - LAG_FORWARD

            @pl.when((f >= 0) & (lax.rem(f + 6, 2) != side))
            def _():
                c_fwd(f).wait_recv()
                c_end(f).start()
                c_share(f).start()

            return carry

        lax.fori_loop(0, steps + LAG_FORWARD, run, 0)

    def finish(k, carry):
        c_share(k).wait_recv()
        c_prt(k).wait_send()
        c_share(k).wait_send()

        @pl.when(is_end)
        def _():
            c_up(k).wait_send()

        @pl.when(is_mid)
        def _():
            c_end(k).wait_send()

            @pl.when(lax.rem(k, 2) != side)
            def _():
                c_mid(k).wait_send()

            @pl.when(lax.rem(k, 2) == side)
            def _():
                c_fwd(k).wait_send()

        return carry

    lax.fori_loop(0, steps, finish, 0)
    flush = pltpu.make_async_copy(tot, out_ref, s_out)
    flush.start()
    flush.wait()


def group_sum(stacked):
    count, size, hidden = stacked.shape
    total = count * size
    half = total // 2
    steps = half // CHUNK
    dma = pltpu.SemaphoreType.DMA((steps,))
    return pl.pallas_call(
        reduce_kernel,
        in_specs=[pl.BlockSpec(memory_space=pltpu.VMEM)],
        out_specs=pl.BlockSpec(memory_space=pl.ANY),
        out_shape=jax.ShapeDtypeStruct((total, hidden), F32),
        scratch_shapes=[pltpu.VMEM((half, hidden), F32)] * 4 + [pltpu.VMEM((total, hidden), F32)] + [dma] * 11 + [pltpu.SemaphoreType.DMA],
        compiler_params=pltpu.CompilerParams(vmem_limit_bytes=VMEM_LIMIT, collective_id=0, has_side_effects=True),
        cost_estimate=cost(10 ** 11, 8 * total * hidden),
        name='group_sum',
    )(stacked.reshape(total, hidden))


def solution(mesh):
    group_size = mesh.shape['ep']
    row_spec = P(('dp', 'ep'), None)
    rep_two = P(None, None)
    rep_one = P(None)
    expert_spec = P('ep', None, None)
    grad_spec = P('dp', None)
    expert_grad_spec = P(('dp', 'ep'), None, None)

    def device_program(x_a, x_b, dy_b, w_q, w_k, w_v, w_o, gain_attn, gain_moe, w_gate, w_up, w_down, expert_a, slot_a, gate_a, expert_b, slot_b, gate_b):
        tokens, hidden = x_a.shape
        num_experts = group_size
        seg = capacity_of(tokens, 1, num_experts)
        half = seg // 3
        w_gate, w_up, w_down = w_gate[0], w_up[0], w_down[0]

        def move(rows):
            return lax.all_to_all(rows.reshape(group_size, seg, hidden), 'ep', 0, 0, tiled=True).reshape(group_size * seg, hidden)

        tables = (expert_a, slot_a, expert_b, slot_b)
        pos_a, pos_b, h_a, pack_a, h_b, *rest = head(x_a, x_b, dy_b, gate_b, tables, (w_q, w_k, w_v, w_o), gain_attn, gain_moe, group_size, seg)
        *saved_b, d_out_b, recv_b = rest
        pos_col_a, pos_col_b = pos_a.reshape(tokens, 1), pos_b.reshape(tokens, 1)
        recv_a = move(pack_a)
        n_b, ids_b = active_blocks(recv_b, half)
        d_in_b, u_c, d_c, act_b, d_zg, d_zu = ffn_backward(n_b, ids_b, recv_b, d_out_b, w_gate, w_up, w_down, half)
        d_back = move(d_in_b)
        n_a, ids_a = active_blocks(recv_a, half)
        o_a = ffn_forward(n_a, ids_a, recv_a, w_gate, w_up, w_down, half)
        back_a = move(o_a)
        d_wgate, d_wup, d_wdown = ffn_grads(n_b, u_c, d_c, act_b, d_zg, d_zu, half)

        d_x, attn_grads = attn_backward(num_experts, x_b, h_b, dy_b, saved_b, d_back, pos_col_b, w_q, w_k, w_v, w_o, gain_attn, gain_moe)
        attn_grads = group_sum(attn_grads)
        y_a, *attn_grads = combine(num_experts, h_a, back_a, pos_col_a, gate_a, attn_grads)
        return (y_a, d_x, *attn_grads, d_wgate[None], d_wup[None], d_wdown[None])

    return jax.shard_map(device_program, mesh=mesh, in_specs=(row_spec, row_spec, row_spec, rep_two, rep_two, rep_two, rep_two, rep_one, rep_one, expert_spec, expert_spec, expert_spec, row_spec, row_spec, row_spec, row_spec, row_spec, row_spec), out_specs=(row_spec, row_spec, grad_spec, grad_spec, grad_spec, grad_spec, expert_grad_spec, expert_grad_spec, expert_grad_spec), check_vma=False)
```
